32 devices in a mesh: dp: 4 (over y, core), slab: 8 (over z, x).
Axes of the slice: x: 2, y: 2, z: 4, core: 2. Of those that a mesh axis runs over, the one named last changes fastest.
Arguments:
- acts: bfloat16 [4, 32, 8, 128, 128], P('dp', None, 'slab'), may hold values from -24 to 24
- grads: bfloat16 [4, 32, 8, 128, 128], P('dp', None, 'slab'), may hold values from -6 to 6
- picks: int32 [4, 4096], P('dp', 'slab'), may hold values from 0 to 31
Outputs:
- weight_grad: float32 [32, 864], replicated
- update: float32 [32, 864], replicated
The draws below stay inside these ranges and needn't reach their ends.
Inputs may be any that keep to these rules, and one draw needn't show every extreme that they name: `picks`: one cell is sampled in each aligned block of 32 of a device's cells, counted plane by plane, row by row, column by column; entry e of a device's 512 entries belongs to block e.
All inputs are finite; a program needn't handle non-finite values.
Results may differ from the reference program's by a relative error of at most 0.0003.
Values may be sent and summed in bfloat16 or wider, within the bound.
A program may use at most 128 MiB of HBM per device.

```python
import math
import jax
import jax.numpy as jnp
from jax import lax

CIN = 32
COUT = 32
PL = 1
H = 128
W = 128
SAMP_DEV = 512
VOLS = 4
DEPTH = 8
N_SLAB = 8


def draw_acts(key, part):
    first, second = jax.random.split(key, 2)
    shape = (VOLS, CIN, DEPTH, H, W)
    height_frac = jnp.arange(DEPTH, dtype=jnp.float32) / (DEPTH - 1)
    rising = jnp.sqrt(1.0 + 2.0 * height_frac)[None, None, :, None, None]
    channel_scale = jnp.exp(jax.random.uniform(first, (CIN,), minval=math.log(0.35), maxval=math.log(3.5)))
    values = jax.random.normal(second, shape, dtype=jnp.float32)
    result = values * channel_scale[None, :, None, None, None] * rising
    return jnp.clip(result, -24.0, 24.0).astype(jnp.bfloat16)


def set_ends(values, key, smallest, top_value):
    longest = values.shape.index(max(values.shape))
    spots = []
    for shift in (0, 1):
        where = [jax.random.randint(jax.random.fold_in(key, axis), (), 0, length) for axis, length in enumerate(values.shape)]
        where[longest] = (where[longest] + shift) % values.shape[longest]
        spots.append(tuple(where))
    return values.at[spots[0]].set(smallest).at[spots[1]].set(top_value)


def block_levels(own_key, shape, cuts, smallest, top_value):
    def one(dim, parts):
        heights = jax.random.uniform(jax.random.fold_in(jax.random.fold_in(own_key, 6), dim), (parts,), jnp.float32, smallest / len(cuts), top_value / len(cuts))
        return jnp.repeat(jnp.exp(heights), shape[dim] // parts).reshape((-1,) + (1,) * (len(shape) - dim - 1))

    level = one(*cuts[0])
    for cut in cuts[1:]:
        level = level * one(*cut)
    return level


def normal_values(stream_key, dims, scale, most, pieces=(), held_as=jnp.bfloat16):
    loudness = block_levels(stream_key, dims, pieces, -0.22, 0.18) if pieces else 1.0
    values = jax.random.normal(stream_key, dims, jnp.float32) * scale * loudness
    return jnp.minimum(jnp.maximum(values, -most), most).astype(held_as)


def setup_inputs(seed: int = 0) -> dict:
    key_of = jax.random.split(jax.random.key(seed), 4)
    acts = draw_acts(jax.random.fold_in(key_of[3], 71), 0)
    grads = normal_values(key_of[1], (VOLS, COUT, DEPTH, H, W), 1.0, 6.0, ((0, 4), (2, 8)))
    picks = set_ends(jax.random.randint(key_of[2], (VOLS, SAMP_DEV * N_SLAB), 0, 32), jax.random.fold_in(key_of[2], 1), 0, 31).astype(jnp.int32)
    return dict(acts=acts, grads=grads, picks=picks)


epsilon = 1e-06
damping = 0.1
trust_region_limit = 0.3
learning_rate = 0.01

def cholesky_apply(factor, values):
    halfway = lax.linalg.triangular_solve(factor, values, left_side=True, lower=True)
    return lax.linalg.triangular_solve(factor, halfway, left_side=True, lower=True, transpose_a=True)

def reference(acts, grads, picks):
    volumes, channels, depth, height, kernel_extent = acts.shape
    outputs = grads.shape[1]
    plane_size = (height + 2) * (kernel_extent + 2)
    shifts = jnp.array([along_z * plane_size + along_y * (kernel_extent + 2) + along_x for along_z in range(3) for along_y in range(3) for along_x in range(3)], dtype=jnp.int32)
    highest = lax.Precision.HIGHEST

    def one_volume(inputs):
        volume, grad_volume, volume_picks = inputs
        padded = jnp.pad(volume, ((0, 0), (1, 1), (1, 1), (1, 1)))
        grad_rows = grad_volume.reshape(outputs, -1)
        products = []
        for offset in range(27):
            along_z, along_y, along_x = (offset // 9, offset // 3 % 3, offset % 3)
            shifted = padded[:, along_z:along_z + depth, along_y:along_y + height, along_x:along_x + kernel_extent].reshape(channels, -1)
            products.append(lax.dot_general(grad_rows.astype(jnp.float32), shifted.astype(jnp.float32), (((1,), (1,)), ((), ())), preferred_element_type=jnp.float32))
        gradient_portion = jnp.concatenate(products, axis=1)
        sample_index = jnp.arange(volume_picks.shape[0], dtype=jnp.int32)
        position = sample_index % SAMP_DEV * 32 + volume_picks
        plane_index = sample_index // SAMP_DEV * PL + position // (height * kernel_extent)
        row_index = position // kernel_extent % height
        column_index = position % kernel_extent
        base_index = plane_index * plane_size + row_index * (kernel_extent + 2) + column_index
        flat_index = (shifts[:, None] + base_index[None, :]).reshape(-1).astype(jnp.int32)
        input_patches = jnp.take(padded.reshape(channels, -1), flat_index, axis=1).reshape(channels, 27, -1).astype(jnp.float32)
        gram = jnp.einsum('cks,dls->kcld', input_patches, input_patches, precision=highest).reshape(27 * channels, 27 * channels)
        grad_index = (plane_index * (height * kernel_extent) + row_index * kernel_extent + column_index).astype(jnp.int32)
        grad_samples = jnp.take(grad_rows, grad_index, axis=1).astype(jnp.float32)
        gradient_gram_matrix = jnp.dot(grad_samples, grad_samples.T, precision=highest)
        return (gradient_portion, gram, gradient_gram_matrix)
    grad_parts, grams, grad_grams = lax.map(one_volume, (acts, grads, picks))
    positions = volumes * depth * height * kernel_extent
    samples = picks.shape[0] * picks.shape[1]
    weight_grad = lax.optimization_barrier(jnp.sum(grad_parts, axis=0)) / math.sqrt(positions)
    factor_acts = lax.optimization_barrier(jnp.sum(grams, axis=0)) / samples
    factor_grads = lax.optimization_barrier(jnp.sum(grad_grams, axis=0)) / samples
    patch_width = factor_acts.shape[0]
    trace_ratio = jnp.sqrt((jnp.trace(factor_acts) / patch_width + epsilon) / (jnp.trace(factor_grads) / outputs + epsilon))
    damped_activation_factor = factor_acts + trace_ratio * math.sqrt(damping) * jnp.eye(patch_width, dtype=jnp.float32)
    damped_grads = factor_grads + math.sqrt(damping) / trace_ratio * jnp.eye(outputs, dtype=jnp.float32)
    chol_acts = jnp.linalg.cholesky(damped_activation_factor)
    chol_grads = jnp.linalg.cholesky(damped_grads)
    left_solved = cholesky_apply(chol_grads, weight_grad)
    precond = cholesky_apply(chol_acts, left_solved.T).T
    quadratic = jnp.sum(precond * weight_grad)
    clip_factor = jnp.minimum(1.0, jnp.sqrt(trust_region_limit / (learning_rate ** 2 * quadratic)))
    return (weight_grad, clip_factor * precond)
```

```python
import functools
import math

import jax
import jax.numpy as jnp
from jax import lax
from jax.experimental import pallas as pl
from jax.experimental.pallas import tpu as pltpu
from jax.sharding import PartitionSpec as P

epsilon = 1e-06
damping = 0.1
trust_region_limit = 0.3
learning_rate = 0.01
BLOCK = 128
CHUNK = 1024
NT = (((1,), (1,)), ((), ()))


def local_kernel(width, own, before, after, grads, targets, out, apad, samples, wsum):
    channels, cells = own.shape
    outputs = grads.shape[0]
    per_chunk = targets.shape[0] // 3
    rows = 27 * channels
    total = samples.shape[0]
    third = 9 * channels
    for a, plane in enumerate((before, own, after)):
        apad[a * channels : (a + 1) * channels, width : width + cells] = plane[...]
    apad[:, 0:width] = jnp.zeros((3 * channels, width), apad.dtype)
    apad[:, width + cells :] = jnp.zeros((3 * channels, width), apad.dtype)
    lane = lax.broadcasted_iota(jnp.int32, (outputs, CHUNK), 1) % width
    position = lax.broadcasted_iota(jnp.int32, (3 * per_chunk, CHUNK), 1)
    sums = jnp.zeros((third, 3 * outputs), jnp.float32)
    for k in range(cells // CHUNK):
        base = k * CHUNK
        g = grads[:, base : base + CHUNK]
        wide = g.astype(jnp.float32)
        left = jnp.where(lane == width - 1, 0.0, pltpu.roll(wide, CHUNK - 1, 1)).astype(g.dtype)
        right = jnp.where(lane == 0, 0.0, pltpu.roll(wide, 1, 1)).astype(g.dtype)
        select = jnp.where(position == targets[:, k : k + 1] - base, 1.0, 0.0).astype(g.dtype)
        lhs = jnp.concatenate(
            [apad[:, base + b * width : base + b * width + CHUNK] for b in range(3)] + [g], axis=0
        )
        rhs = jnp.concatenate([left, g, right, select], axis=0)
        both = lax.dot_general(lhs, rhs, NT, preferred_element_type=jnp.float32)
        sums += both[:third, : 3 * outputs]
        where = slice(k * per_chunk, (k + 1) * per_chunk)
        for c in range(3):
            start = 3 * outputs + c * per_chunk
            samples[c * third : (c + 1) * third, where] = both[:third, start : start + per_chunk]
        start = 3 * outputs + per_chunk
        samples[rows : rows + outputs, where] = both[third:, start : start + per_chunk]
    offset = BLOCK - outputs
    for c in range(3):
        wsum[c * third : (c + 1) * third, offset:] = sums[:, c * outputs : (c + 1) * outputs]
    count = total // BLOCK
    r = lax.broadcasted_iota(jnp.int32, (BLOCK, BLOCK), 0)
    l = lax.broadcasted_iota(jnp.int32, (BLOCK, BLOCK), 1)
    vectors = samples[...].astype(jnp.bfloat16)
    slot = 0
    for i in range(count):
        gram = lax.dot_general(
            vectors[i * BLOCK : (i + 1) * BLOCK],
            vectors[i * BLOCK :],
            NT,
            preferred_element_type=jnp.float32,
        )
        for j in range(i, count):
            block = gram[:, (j - i) * BLOCK : (j - i + 1) * BLOCK]
            if j == count - 1:
                weights = wsum[i * BLOCK : (i + 1) * BLOCK, :]
                block = jnp.where((l >= offset) & (r + i * BLOCK < rows), weights, block)
            out[slot] = block
            slot += 1


def split3(value):
    first = value.astype(jnp.bfloat16)
    rest = value - first.astype(jnp.float32)
    second = rest.astype(jnp.bfloat16)
    third = (rest - second.astype(jnp.float32)).astype(jnp.bfloat16)
    return first, second, third


def solve_kernel(
    positions, sample_total, channels, outputs, total, weight_out, update_out,
    a1, a2, a3, pieces, x_ref, r_ref, p_ref, w_ref, inv_ref
):
    rows = 27 * channels
    size = a1.shape[0]
    count = size // BLOCK
    offset = BLOCK - outputs
    r = lax.broadcasted_iota(jnp.int32, (BLOCK, BLOCK), 0)
    l = lax.broadcasted_iota(jnp.int32, (BLOCK, BLOCK), 1)
    slots = {}
    for i in range(count):
        for j in range(i, count):
            slots[i, j] = len(slots)
    diagonals = [
        jnp.sum(jnp.where(r == l, total[slots[i, i]], 0.0), axis=1, keepdims=True)
        for i in range(count)
    ]
    column = lax.broadcasted_iota(jnp.int32, (BLOCK, 1), 0)
    trace_a = jnp.zeros((1, 1), jnp.float32)
    trace_g = jnp.zeros((1, 1), jnp.float32)
    for i in range(count):
        inside = column + i * BLOCK < rows
        trace_a += jnp.sum(jnp.where(inside, diagonals[i], 0.0), axis=0, keepdims=True)
        trace_g += jnp.sum(jnp.where(inside, 0.0, diagonals[i]), axis=0, keepdims=True)
    ratio = jnp.sqrt(
        (trace_a / sample_total / rows + epsilon) / (trace_g / sample_total / outputs + epsilon)
    )
    shift_a = ratio * math.sqrt(damping)
    shift_g = math.sqrt(damping) / ratio
    for i in range(count):
        inside = column + i * BLOCK < rows
        inv_ref[i * BLOCK : (i + 1) * BLOCK, :] = 1.0 / jnp.where(
            inside, diagonals[i] / sample_total + shift_a, 1.0
        )
        for j in range(i, count):
            block = total[slots[i, j]] / sample_total
            if j == count - 1:
                w_ref[i * BLOCK : (i + 1) * BLOCK, :] = (
                    total[slots[i, j]][:, offset:] / math.sqrt(positions)
                )
                block = jnp.where((r + i * BLOCK < rows) & (l + j * BLOCK < rows), block, 0.0)
            if i == j:
                shift = jnp.where(r + i * BLOCK < rows, shift_a, 1.0)
                block = jnp.where(r == l, block + shift, block)
            here = (slice(i * BLOCK, (i + 1) * BLOCK), slice(j * BLOCK, (j + 1) * BLOCK))
            for ref, part in zip((a1, a2, a3), split3(block)):
                ref[here] = part
            if i != j:
                for ref, part in zip((a1, a2, a3), split3(block.T)):
                    ref[here[1], here[0]] = part
    w_ref[rows:, :] = jnp.zeros((size - rows, outputs), jnp.float32)

    gr = lax.broadcasted_iota(jnp.int32, (outputs, outputs), 0)
    gc = lax.broadcasted_iota(jnp.int32, (outputs, outputs), 1)
    factor = total[slots[count - 1, count - 1]][offset:, offset:] / sample_total
    factor = jnp.where(gr == gc, factor + shift_g, factor)

    def eliminate(k, m):
        row = jnp.sum(jnp.where(gr == k, m, 0.0), axis=0, keepdims=True)
        col = jnp.sum(jnp.where(gc == k, m, 0.0), axis=1, keepdims=True)
        pivot = jnp.sum(jnp.where(gr[:, :1] == k, col, 0.0), axis=0, keepdims=True)
        inverse = 1.0 / pivot
        scaled = row * inverse
        rest = m - col * scaled
        rest = jnp.where(gr == k, scaled, rest)
        rest = jnp.where(gc == k, -col * inverse, rest)
        return jnp.where((gr == k) & (gc == k), inverse, rest)

    inverse_g = lax.fori_loop(0, outputs, eliminate, factor)
    weights = w_ref[...]
    rhs = jnp.dot(
        weights, inverse_g, precision=lax.Precision.HIGHEST, preferred_element_type=jnp.float32
    )
    top = jnp.max(jnp.abs(rhs), axis=0, keepdims=True)
    top = jnp.where(top > 0.0, top, 1.0)
    residual = rhs / top
    x_ref[...] = jnp.zeros_like(x_ref)
    r_ref[...] = residual
    z = residual * inv_ref[...]
    p_ref[...] = z
    rz0 = jnp.sum(residual * z, axis=0, keepdims=True)
    goal = rz0 * 1e-16

    def unfinished(state):
        step, rz = state
        return (jnp.max(jnp.where(rz > goal, 1.0, 0.0)) > 0.0) & (step < 8 * size)

    def iterate(state):
        step, rz = state
        p = p_ref[...]
        for n, part in enumerate(split3(p)):
            pieces[:, n * outputs : (n + 1) * outputs] = part
        product = jnp.dot(a1[...], pieces[...], preferred_element_type=jnp.float32)
        second = jnp.dot(a2[...], pieces[:, : 2 * outputs], preferred_element_type=jnp.float32)
        third = jnp.dot(a3[...], pieces[:, :outputs], preferred_element_type=jnp.float32)
        q = (
            product[:, 2 * outputs :] + second[:, outputs:] + third
        ) + (product[:, outputs : 2 * outputs] + second[:, :outputs]) + product[:, :outputs]
        pq = jnp.sum(p * q, axis=0, keepdims=True)
        alpha = jnp.where(pq > 0.0, rz / jnp.where(pq > 0.0, pq, 1.0), 0.0)
        x_ref[...] += alpha * p
        left = r_ref[...] - alpha * q
        r_ref[...] = left
        preconditioned = left * inv_ref[...]
        after = jnp.sum(left * preconditioned, axis=0, keepdims=True)
        beta = jnp.where(rz > 0.0, after / jnp.where(rz > 0.0, rz, 1.0), 0.0)
        p_ref[...] = preconditioned + beta * p
        return step + 1, after

    lax.while_loop(unfinished, iterate, (jnp.int32(0), rz0))
    precond = x_ref[...] * top
    quadratic = jnp.sum(
        jnp.sum(precond * weights, axis=0, keepdims=True), axis=1, keepdims=True
    )
    clip = jnp.minimum(1.0, jnp.sqrt(trust_region_limit / (learning_rate**2 * quadratic)))
    flat_w = weights.T
    flat_u = (precond * clip).T
    for c in range(3):
        for b in range(3):
            for a in range(3):
                source = (c * 9 + b * 3 + a) * channels
                dest = (a * 9 + b * 3 + c) * channels
                weight_out[:, dest : dest + channels] = flat_w[:, source : source + channels]
                update_out[:, dest : dest + channels] = flat_u[:, source : source + channels]


def halo(plane):
    size = lax.axis_size("slab")
    pairs = [(i, i ^ 1) for i in range(size) if i ^ 1 < size]
    relays = [(i, i + 2) for i in range(0, size - 2, 2)] + [(i, i - 2) for i in range(3, size, 2)]
    swapped, relayed = [], []
    for part in jnp.split(plane, 4, axis=0):
        got = lax.ppermute(part, "slab", pairs)
        swapped.append(got)
        relayed.append(lax.ppermute(got, "slab", relays))
    swapped = jnp.concatenate(swapped, axis=0)
    relayed = jnp.concatenate(relayed, axis=0)
    even = lax.axis_index("slab") % 2 == 0
    return jnp.where(even, relayed, swapped), jnp.where(even, swapped, relayed)


def shards(acts, grads, picks):
    volumes, channels, planes, height, width = acts.shape
    outputs = grads.shape[1]
    cells = height * width
    own = acts.reshape(channels, cells)
    rows = grads.reshape(outputs, cells)
    before, after = halo(own)
    samples = picks.shape[1]
    chunks = cells // CHUNK
    position = jnp.arange(samples, dtype=jnp.int32) * 32 + picks.reshape(samples)
    column = position % width
    targets = jnp.stack(
        [
            jnp.where((column + d >= 0) & (column + d < width), position + d, -1)
            for d in (-1, 0, 1)
        ]
    )
    targets = targets.reshape(3, chunks, samples // chunks).transpose(0, 2, 1)
    targets = targets.reshape(3 * (samples // chunks), chunks)
    size = 27 * channels + outputs
    count = size // BLOCK
    blocks = count * (count + 1) // 2
    partial = pl.pallas_call(
        functools.partial(local_kernel, width),
        out_shape=jax.ShapeDtypeStruct((blocks, BLOCK, BLOCK), jnp.float32),
        in_specs=[pl.BlockSpec(memory_space=pltpu.VMEM)] * 5,
        out_specs=pl.BlockSpec(memory_space=pltpu.VMEM),
        scratch_shapes=[
            pltpu.VMEM((3 * channels, cells + 2 * width), jnp.bfloat16),
            pltpu.VMEM((size, samples), jnp.float32),
            pltpu.VMEM((size, BLOCK), jnp.float32),
        ],
        compiler_params=pltpu.CompilerParams(vmem_limit_bytes=48 * 1024 * 1024),
        name="local_sums",
    )(own, before, after, rows, targets)
    total = lax.psum(partial, ("dp", "slab"))
    everyone = lax.axis_size("dp") * lax.axis_size("slab") * volumes
    return pl.pallas_call(
        functools.partial(
            solve_kernel, everyone * planes * cells, everyone * samples, channels, outputs
        ),
        out_shape=[jax.ShapeDtypeStruct((outputs, 27 * channels), jnp.float32)] * 2,
        in_specs=[pl.BlockSpec(memory_space=pltpu.VMEM)],
        out_specs=[pl.BlockSpec(memory_space=pltpu.VMEM)] * 2,
        scratch_shapes=[pltpu.VMEM((size, size), jnp.bfloat16)] * 3
        + [pltpu.VMEM((size, 3 * outputs), jnp.bfloat16)]
        + [pltpu.VMEM((size, outputs), jnp.float32)] * 4
        + [pltpu.VMEM((size, 1), jnp.float32)],
        compiler_params=pltpu.CompilerParams(vmem_limit_bytes=48 * 1024 * 1024),
        name="solve",
    )(total)


def solution(mesh):
    return jax.shard_map(
        shards,
        mesh=mesh,
        in_specs=(
            P("dp", None, "slab", None, None),
            P("dp", None, "slab", None, None),
            P("dp", "slab"),
        ),
        out_specs=(P(), P()),
        check_vma=False,
    )
```

```python
import functools
import math

import jax
import jax.numpy as jnp
from jax import lax
from jax.experimental import pallas as pl
from jax.experimental.pallas import tpu as pltpu
from jax.sharding import PartitionSpec as P

epsilon = 1e-06
damping = 0.1
trust_region_limit = 0.3
learning_rate = 0.01
BLOCK = 128
CHUNK = 1024
NT = (((1,), (1,)), ((), ()))


def local_kernel(width, own, before, after, grads, targets, out, apad, samples, wsum):
    channels, cells = own.shape
    outputs = grads.shape[0]
    per_chunk = targets.shape[0] // 3
    rows = 27 * channels
    total = samples.shape[0]
    third = 9 * channels
    for a, plane in enumerate((before, own, after)):
        apad[a * channels : (a + 1) * channels, width : width + cells] = plane[...]
    apad[:, 0:width] = jnp.zeros((3 * channels, width), apad.dtype)
    apad[:, width + cells :] = jnp.zeros((3 * channels, width), apad.dtype)
    lane = lax.broadcasted_iota(jnp.int32, (outputs, CHUNK), 1) % width
    position = lax.broadcasted_iota(jnp.int32, (3 * per_chunk, CHUNK), 1)
    sums = jnp.zeros((third, 3 * outputs), jnp.float32)
    for k in range(cells // CHUNK):
        base = k * CHUNK
        g = grads[:, base : base + CHUNK]
        wide = g.astype(jnp.float32)
        left = jnp.where(lane == width - 1, 0.0, pltpu.roll(wide, CHUNK - 1, 1)).astype(g.dtype)
        right = jnp.where(lane == 0, 0.0, pltpu.roll(wide, 1, 1)).astype(g.dtype)
        select = jnp.where(position == targets[:, k : k + 1] - base, 1.0, 0.0).astype(g.dtype)
        lhs = jnp.concatenate(
            [apad[:, base + b * width : base + b * width + CHUNK] for b in range(3)] + [g], axis=0
        )
        rhs = jnp.concatenate([left, g, right, select], axis=0)
        both = lax.dot_general(lhs, rhs, NT, preferred_element_type=jnp.float32)
        sums += both[:third, : 3 * outputs]
        where = slice(k * per_chunk, (k + 1) * per_chunk)
        for c in range(3):
            start = 3 * outputs + c * per_chunk
            samples[c * third : (c + 1) * third, where] = both[:third, start : start + per_chunk]
        start = 3 * outputs + per_chunk
        samples[rows : rows + outputs, where] = both[third:, start : start + per_chunk]
    offset = BLOCK - outputs
    for c in range(3):
        wsum[c * third : (c + 1) * third, offset:] = sums[:, c * outputs : (c + 1) * outputs]
    count = total // BLOCK
    r = lax.broadcasted_iota(jnp.int32, (BLOCK, BLOCK), 0)
    l = lax.broadcasted_iota(jnp.int32, (BLOCK, BLOCK), 1)
    vectors = samples[...].astype(jnp.bfloat16)
    slot = 0
    for i in range(count):
        gram = lax.dot_general(
            vectors[i * BLOCK : (i + 1) * BLOCK],
            vectors[i * BLOCK :],
            NT,
            preferred_element_type=jnp.float32,
        )
        for j in range(i, count):
            block = gram[:, (j - i) * BLOCK : (j - i + 1) * BLOCK]
            if j == count - 1:
                weights = wsum[i * BLOCK : (i + 1) * BLOCK, :]
                block = jnp.where((l >= offset) & (r + i * BLOCK < rows), weights, block)
            out[slot] = block
            slot += 1


def split3(value):
    first = value.astype(jnp.bfloat16)
    rest = value - first.astype(jnp.float32)
    second = rest.astype(jnp.bfloat16)
    third = (rest - second.astype(jnp.float32)).astype(jnp.bfloat16)
    return first, second, third


def solve_kernel(
    positions, sample_total, channels, outputs, total, weight_out, update_out,
    a1, a2, a3, pieces, x_ref, r_ref, p_ref, w_ref, inv_ref
):
    rows = 27 * channels
    size = a1.shape[0]
    count = size // BLOCK
    offset = BLOCK - outputs
    r = lax.broadcasted_iota(jnp.int32, (BLOCK, BLOCK), 0)
    l = lax.broadcasted_iota(jnp.int32, (BLOCK, BLOCK), 1)
    slots = {}
    for i in range(count):
        for j in range(i, count):
            slots[i, j] = len(slots)
    diagonals = [
        jnp.sum(jnp.where(r == l, total[slots[i, i]], 0.0), axis=1, keepdims=True)
        for i in range(count)
    ]
    column = lax.broadcasted_iota(jnp.int32, (BLOCK, 1), 0)
    trace_a = jnp.zeros((1, 1), jnp.float32)
    trace_g = jnp.zeros((1, 1), jnp.float32)
    for i in range(count):
        inside = column + i * BLOCK < rows
        trace_a += jnp.sum(jnp.where(inside, diagonals[i], 0.0), axis=0, keepdims=True)
        trace_g += jnp.sum(jnp.where(inside, 0.0, diagonals[i]), axis=0, keepdims=True)
    ratio = jnp.sqrt(
        (trace_a / sample_total / rows + epsilon) / (trace_g / sample_total / outputs + epsilon)
    )
    shift_a = ratio * math.sqrt(damping)
    shift_g = math.sqrt(damping) / ratio
    for i in range(count):
        inside = column + i * BLOCK < rows
        inv_ref[i * BLOCK : (i + 1) * BLOCK, :] = 1.0 / jnp.where(
            inside, diagonals[i] / sample_total + shift_a, 1.0
        )
        for j in range(i, count):
            block = total[slots[i, j]] / sample_total
            if j == count - 1:
                w_ref[i * BLOCK : (i + 1) * BLOCK, :] = (
                    total[slots[i, j]][:, offset:] / math.sqrt(positions)
                )
                block = jnp.where((r + i * BLOCK < rows) & (l + j * BLOCK < rows), block, 0.0)
            if i == j:
                shift = jnp.where(r + i * BLOCK < rows, shift_a, 1.0)
                block = jnp.where(r == l, block + shift, block)
            here = (slice(i * BLOCK, (i + 1) * BLOCK), slice(j * BLOCK, (j + 1) * BLOCK))
            for ref, part in zip((a1, a2, a3), split3(block)):
                ref[here] = part
            if i != j:
                for ref, part in zip((a1, a2, a3), split3(block.T)):
                    ref[here[1], here[0]] = part
    w_ref[rows:, :] = jnp.zeros((size - rows, outputs), jnp.float32)

    gr = lax.broadcasted_iota(jnp.int32, (outputs, outputs), 0)
    gc = lax.broadcasted_iota(jnp.int32, (outputs, outputs), 1)
    factor = total[slots[count - 1, count - 1]][offset:, offset:] / sample_total
    factor = jnp.where(gr == gc, factor + shift_g, factor)

    def eliminate(k, m):
        row = jnp.sum(jnp.where(gr == k, m, 0.0), axis=0, keepdims=True)
        col = jnp.sum(jnp.where(gc == k, m, 0.0), axis=1, keepdims=True)
        pivot = jnp.sum(jnp.where(gr[:, :1] == k, col, 0.0), axis=0, keepdims=True)
        inverse = 1.0 / pivot
        scaled = row * inverse
        rest = m - col * scaled
        rest = jnp.where(gr == k, scaled, rest)
        rest = jnp.where(gc == k, -col * inverse, rest)
        return jnp.where((gr == k) & (gc == k), inverse, rest)

    inverse_g = lax.fori_loop(0, outputs, eliminate, factor)
    weights = w_ref[...]
    rhs = jnp.dot(
        weights, inverse_g, precision=lax.Precision.HIGHEST, preferred_element_type=jnp.float32
    )
    top = jnp.max(jnp.abs(rhs), axis=0, keepdims=True)
    top = jnp.where(top > 0.0, top, 1.0)
    residual = rhs / top
    x_ref[...] = jnp.zeros_like(x_ref)
    r_ref[...] = residual
    z = residual * inv_ref[...]
    p_ref[...] = z
    rz0 = jnp.sum(residual * z, axis=0, keepdims=True)
    goal = rz0 * 1e-16

    def unfinished(state):
        step, rz = state
        return (jnp.max(jnp.where(rz > goal, 1.0, 0.0)) > 0.0) & (step < 8 * size)

    def iterate(state):
        step, rz = state
        p = p_ref[...]
        for n, part in enumerate(split3(p)):
            pieces[:, n * outputs : (n + 1) * outputs] = part
        product = jnp.dot(a1[...], pieces[...], preferred_element_type=jnp.float32)
        second = jnp.dot(a2[...], pieces[:, : 2 * outputs], preferred_element_type=jnp.float32)
        third = jnp.dot(a3[...], pieces[:, :outputs], preferred_element_type=jnp.float32)
        q = (
            product[:, 2 * outputs :] + second[:, outputs:] + third
        ) + (product[:, outputs : 2 * outputs] + second[:, :outputs]) + product[:, :outputs]
        pq = jnp.sum(p * q, axis=0, keepdims=True)
        alpha = jnp.where(pq > 0.0, rz / jnp.where(pq > 0.0, pq, 1.0), 0.0)
        x_ref[...] += alpha * p
        left = r_ref[...] - alpha * q
        r_ref[...] = left
        preconditioned = left * inv_ref[...]
        after = jnp.sum(left * preconditioned, axis=0, keepdims=True)
        beta = jnp.where(rz > 0.0, after / jnp.where(rz > 0.0, rz, 1.0), 0.0)
        p_ref[...] = preconditioned + beta * p
        return step + 1, after

    lax.while_loop(unfinished, iterate, (jnp.int32(0), rz0))
    precond = x_ref[...] * top
    quadratic = jnp.sum(
        jnp.sum(precond * weights, axis=0, keepdims=True), axis=1, keepdims=True
    )
    clip = jnp.minimum(1.0, jnp.sqrt(trust_region_limit / (learning_rate**2 * quadratic)))
    flat_w = weights.T
    flat_u = (precond * clip).T
    for c in range(3):
        for b in range(3):
            for a in range(3):
                source = (c * 9 + b * 3 + a) * channels
                dest = (a * 9 + b * 3 + c) * channels
                weight_out[:, dest : dest + channels] = flat_w[:, source : source + channels]
                update_out[:, dest : dest + channels] = flat_u[:, source : source + channels]


MESH = pl.DeviceIdType.MESH


def bit_orders(dp, slab):
    core = [("dp", 1)] if dp > 1 else []
    along_y = [("dp", 1 << n) for n in range(1, dp.bit_length() - 1)]
    along_x = [("slab", 1)] if slab > 1 else []
    along_z = [("slab", 1 << n) for n in range(1, slab.bit_length() - 1)]
    groups = [along_x, along_y, along_z]
    return [core + groups[n] + groups[(n + 1) % 3] + groups[(n + 2) % 3] for n in range(3)]


def portion_plan(rows, orders):
    unit = rows // 14
    sizes = [5 * unit, 5 * unit, rows - 10 * unit]
    plan, start = [], 0
    for size, order in zip(sizes, orders):
        stages, length = [], size
        for bit in order:
            halves = length % 16 == 0
            length = length // 2 if halves else length
            stages.append((bit, length, halves))
        plan.append((start, size, stages))
        start += size
    return plan


def sum_kernel(plan, value, out, work, *scratch):
    stages = len(plan[0][2])
    recv = [scratch[n * stages : (n + 1) * stages] for n in range(len(plan))]
    send_sem, recv_sem = scratch[len(plan) * stages :]
    me = {"dp": lax.axis_index("dp"), "slab": lax.axis_index("slab")}

    def bit_of(bit):
        return (me[bit[0]] // bit[1]) % 2

    def partner(bit):
        there = dict(me)
        there[bit[0]] = me[bit[0]] + bit[1] * (1 - 2 * bit_of(bit))
        return (there["dp"], there["slab"])

    barrier = pltpu.get_barrier_semaphore()
    for bit, _, _ in plan[0][2]:
        pl.semaphore_signal(barrier, inc=1, device_id=partner(bit), device_id_type=MESH)
    pl.semaphore_wait(barrier, stages)

    first = [[start] for start, _, _ in plan]

    def window(start, length):
        return pl.ds(pl.multiple_of(start, 8), length)

    def begin(n, s):
        bit, length, halves = plan[n][2][s]
        before = first[n][s]
        mine = before + bit_of(bit) * length if halves else before
        other = before + (1 - bit_of(bit)) * length if halves else before
        first[n].append(mine)
        source = value if s == 0 else work
        copy = pltpu.make_async_remote_copy(
            src_ref=source.at[window(other, length)],
            dst_ref=recv[n][s],
            send_sem=send_sem.at[0, n, s],
            recv_sem=recv_sem.at[0, n, s],
            device_id=partner(bit),
            device_id_type=MESH,
        )
        copy.start()
        return copy

    flying = [begin(n, 0) for n in range(len(plan))]
    for s in range(stages):
        for n in range(len(plan)):
            _, length, _ = plan[n][2][s]
            flying[n].wait()
            here = window(first[n][s + 1], length)
            source = value if s == 0 else work
            target = work if s + 1 < stages else out
            target[here, :] = source[here, :] + recv[n][s][...]
            if s + 1 < stages:
                flying[n] = begin(n, s + 1)

    def spread(n, s):
        bit, length, _ = plan[n][2][s]
        here = window(first[n][s + 1], length)
        copy = pltpu.make_async_remote_copy(
            src_ref=out.at[here],
            dst_ref=out.at[here],
            send_sem=send_sem.at[1, n, s],
            recv_sem=recv_sem.at[1, n, s],
            device_id=partner(bit),
            device_id_type=MESH,
        )
        copy.start()
        return copy

    back = [[s for s in range(stages - 1, -1, -1) if stage[2][s][2]] for stage in plan]
    flying = [spread(n, back[n][0]) for n in range(len(plan))]
    for step in range(max(len(b) for b in back)):
        for n in range(len(plan)):
            if step < len(back[n]):
                flying[n].wait()
                if step + 1 < len(back[n]):
                    flying[n] = spread(n, back[n][step + 1])


def sum_everywhere(value):
    rows, lanes = value.shape
    plan = portion_plan(rows, bit_orders(lax.axis_size("dp"), lax.axis_size("slab")))
    stages = len(plan[0][2])
    buffers = [
        pltpu.VMEM((length, lanes), value.dtype) for _, _, steps in plan for _, length, _ in steps
    ]
    return pl.pallas_call(
        functools.partial(sum_kernel, plan),
        out_shape=jax.ShapeDtypeStruct(value.shape, value.dtype),
        in_specs=[pl.BlockSpec(memory_space=pltpu.VMEM)],
        out_specs=pl.BlockSpec(memory_space=pltpu.VMEM),
        scratch_shapes=[pltpu.VMEM(value.shape, value.dtype)]
        + buffers
        + [pltpu.SemaphoreType.DMA((2, len(plan), stages))] * 2,
        compiler_params=pltpu.CompilerParams(
            collective_id=0, has_side_effects=True, vmem_limit_bytes=24 * 1024 * 1024
        ),
        name="sum_everywhere",
    )(value)


def halo(plane):
    size = lax.axis_size("slab")
    pairs = [(i, i ^ 1) for i in range(size) if i ^ 1 < size]
    relays = [(i, i + 2) for i in range(0, size - 2, 2)] + [(i, i - 2) for i in range(3, size, 2)]
    swapped, relayed = [], []
    for part in jnp.split(plane, 4, axis=0):
        got = lax.ppermute(part, "slab", pairs)
        swapped.append(got)
        relayed.append(lax.ppermute(got, "slab", relays))
    swapped = jnp.concatenate(swapped, axis=0)
    relayed = jnp.concatenate(relayed, axis=0)
    even = lax.axis_index("slab") % 2 == 0
    return jnp.where(even, relayed, swapped), jnp.where(even, swapped, relayed)


def shards(acts, grads, picks):
    volumes, channels, planes, height, width = acts.shape
    outputs = grads.shape[1]
    cells = height * width
    own = acts.reshape(channels, cells)
    rows = grads.reshape(outputs, cells)
    before, after = halo(own)
    samples = picks.shape[1]
    chunks = cells // CHUNK
    position = jnp.arange(samples, dtype=jnp.int32) * 32 + picks.reshape(samples)
    column = position % width
    targets = jnp.stack(
        [
            jnp.where((column + d >= 0) & (column + d < width), position + d, -1)
            for d in (-1, 0, 1)
        ]
    )
    targets = targets.reshape(3, chunks, samples // chunks).transpose(0, 2, 1)
    targets = targets.reshape(3 * (samples // chunks), chunks)
    size = 27 * channels + outputs
    count = size // BLOCK
    blocks = count * (count + 1) // 2
    partial = pl.pallas_call(
        functools.partial(local_kernel, width),
        out_shape=jax.ShapeDtypeStruct((blocks, BLOCK, BLOCK), jnp.float32),
        in_specs=[pl.BlockSpec(memory_space=pltpu.VMEM)] * 5,
        out_specs=pl.BlockSpec(memory_space=pltpu.VMEM),
        scratch_shapes=[
            pltpu.VMEM((3 * channels, cells + 2 * width), jnp.bfloat16),
            pltpu.VMEM((size, samples), jnp.float32),
            pltpu.VMEM((size, BLOCK), jnp.float32),
        ],
        compiler_params=pltpu.CompilerParams(vmem_limit_bytes=48 * 1024 * 1024),
        name="local_sums",
    )(own, before, after, rows, targets)
    total = sum_everywhere(partial.reshape(-1, BLOCK)).reshape(partial.shape)
    everyone = lax.axis_size("dp") * lax.axis_size("slab") * volumes
    return pl.pallas_call(
        functools.partial(
            solve_kernel, everyone * planes * cells, everyone * samples, channels, outputs
        ),
        out_shape=[jax.ShapeDtypeStruct((outputs, 27 * channels), jnp.float32)] * 2,
        in_specs=[pl.BlockSpec(memory_space=pltpu.VMEM)],
        out_specs=[pl.BlockSpec(memory_space=pltpu.VMEM)] * 2,
        scratch_shapes=[pltpu.VMEM((size, size), jnp.bfloat16)] * 3
        + [pltpu.VMEM((size, 3 * outputs), jnp.bfloat16)]
        + [pltpu.VMEM((size, outputs), jnp.float32)] * 4
        + [pltpu.VMEM((size, 1), jnp.float32)],
        compiler_params=pltpu.CompilerParams(vmem_limit_bytes=48 * 1024 * 1024),
        name="solve",
    )(total)


def solution(mesh):
    return jax.shard_map(
        shards,
        mesh=mesh,
        in_specs=(
            P("dp", None, "slab", None, None),
            P("dp", None, "slab", None, None),
            P("dp", "slab"),
        ),
        out_specs=(P(), P()),
        check_vma=False,
    )
```

```python
import functools
import math

import jax
import jax.numpy as jnp
from jax import lax
from jax.experimental import pallas as pl
from jax.experimental.pallas import tpu as pltpu
from jax.sharding import PartitionSpec as P

epsilon = 1e-06
damping = 0.1
trust_region_limit = 0.3
learning_rate = 0.01
BLOCK = 128
CHUNK = 1024
NT = (((1,), (1,)), ((), ()))


def local_kernel(width, own, swapped, relayed, grads, targets, out, apad, samples, wsum):
    channels, cells = own.shape
    outputs = grads.shape[0]
    per_chunk = targets.shape[0] // 3
    rows = 27 * channels
    total = samples.shape[0]
    third = 9 * channels
    odd = lax.axis_index("slab") % 2 == 1
    inner = slice(width, width + cells)
    apad[channels : 2 * channels, inner] = own[...]

    @pl.when(odd)
    def _():
        apad[:channels, inner] = swapped[...]
        apad[2 * channels :, inner] = relayed[...]

    @pl.when(jnp.logical_not(odd))
    def _():
        apad[:channels, inner] = relayed[...]
        apad[2 * channels :, inner] = swapped[...]

    apad[:, 0:width] = jnp.zeros((3 * channels, width), apad.dtype)
    apad[:, width + cells :] = jnp.zeros((3 * channels, width), apad.dtype)
    lane = lax.broadcasted_iota(jnp.int32, (outputs, CHUNK), 1) % width
    position = lax.broadcasted_iota(jnp.int32, (3 * per_chunk, CHUNK), 1)
    sums = jnp.zeros((third, 3 * outputs), jnp.float32)
    for k in range(cells // CHUNK):
        base = k * CHUNK
        g = grads[:, base : base + CHUNK]
        wide = g.astype(jnp.float32)
        left = jnp.where(lane == width - 1, 0.0, pltpu.roll(wide, CHUNK - 1, 1)).astype(g.dtype)
        right = jnp.where(lane == 0, 0.0, pltpu.roll(wide, 1, 1)).astype(g.dtype)
        select = jnp.where(position == targets[:, k : k + 1] - base, 1.0, 0.0).astype(g.dtype)
        lhs = jnp.concatenate(
            [apad[:, base + b * width : base + b * width + CHUNK] for b in range(3)] + [g], axis=0
        )
        rhs = jnp.concatenate([left, g, right, select], axis=0)
        both = lax.dot_general(lhs, rhs, NT, preferred_element_type=jnp.float32)
        sums += both[:third, : 3 * outputs]
        where = slice(k * per_chunk, (k + 1) * per_chunk)
        for c in range(3):
            start = 3 * outputs + c * per_chunk
            samples[c * third : (c + 1) * third, where] = both[:third, start : start + per_chunk]
        start = 3 * outputs + per_chunk
        samples[rows : rows + outputs, where] = both[third:, start : start + per_chunk]
    offset = BLOCK - outputs
    for c in range(3):
        wsum[c * third : (c + 1) * third, offset:] = sums[:, c * outputs : (c + 1) * outputs]
    count = total // BLOCK
    r = lax.broadcasted_iota(jnp.int32, (BLOCK, BLOCK), 0)
    l = lax.broadcasted_iota(jnp.int32, (BLOCK, BLOCK), 1)
    vectors = samples[...].astype(jnp.bfloat16)
    slot = 0
    for i in range(count):
        gram = lax.dot_general(
            vectors[i * BLOCK : (i + 1) * BLOCK],
            vectors[i * BLOCK :],
            NT,
            preferred_element_type=jnp.float32,
        )
        for j in range(i, count):
            block = gram[:, (j - i) * BLOCK : (j - i + 1) * BLOCK]
            if j == count - 1:
                weights = wsum[i * BLOCK : (i + 1) * BLOCK, :]
                block = jnp.where((l >= offset) & (r + i * BLOCK < rows), weights, block)
            out[slot] = block
            slot += 1


def split3(value):
    first = value.astype(jnp.bfloat16)
    rest = value - first.astype(jnp.float32)
    second = rest.astype(jnp.bfloat16)
    third = (rest - second.astype(jnp.float32)).astype(jnp.bfloat16)
    return first, second, third


def solve_kernel(
    positions, sample_total, channels, outputs, total, weight_out, update_out,
    a1, a2, a3, pieces, x_ref, r_ref, p_ref, w_ref, inv_ref
):
    rows = 27 * channels
    size = a1.shape[0]
    count = size // BLOCK
    offset = BLOCK - outputs
    r = lax.broadcasted_iota(jnp.int32, (BLOCK, BLOCK), 0)
    l = lax.broadcasted_iota(jnp.int32, (BLOCK, BLOCK), 1)
    slots = {}
    for i in range(count):
        for j in range(i, count):
            slots[i, j] = len(slots)
    diagonals = [
        jnp.sum(jnp.where(r == l, total[slots[i, i]], 0.0), axis=1, keepdims=True)
        for i in range(count)
    ]
    column = lax.broadcasted_iota(jnp.int32, (BLOCK, 1), 0)
    trace_a = jnp.zeros((1, 1), jnp.float32)
    trace_g = jnp.zeros((1, 1), jnp.float32)
    for i in range(count):
        inside = column + i * BLOCK < rows
        trace_a += jnp.sum(jnp.where(inside, diagonals[i], 0.0), axis=0, keepdims=True)
        trace_g += jnp.sum(jnp.where(inside, 0.0, diagonals[i]), axis=0, keepdims=True)
    ratio = jnp.sqrt(
        (trace_a / sample_total / rows + epsilon) / (trace_g / sample_total / outputs + epsilon)
    )
    shift_a = ratio * math.sqrt(damping)
    shift_g = math.sqrt(damping) / ratio
    for i in range(count):
        inside = column + i * BLOCK < rows
        inv_ref[i * BLOCK : (i + 1) * BLOCK, :] = 1.0 / jnp.where(
            inside, diagonals[i] / sample_total + shift_a, 1.0
        )
        for j in range(i, count):
            block = total[slots[i, j]] / sample_total
            if j == count - 1:
                w_ref[i * BLOCK : (i + 1) * BLOCK, :] = (
                    total[slots[i, j]][:, offset:] / math.sqrt(positions)
                )
                block = jnp.where((r + i * BLOCK < rows) & (l + j * BLOCK < rows), block, 0.0)
            if i == j:
                shift = jnp.where(r + i * BLOCK < rows, shift_a, 1.0)
                block = jnp.where(r == l, block + shift, block)
            here = (slice(i * BLOCK, (i + 1) * BLOCK), slice(j * BLOCK, (j + 1) * BLOCK))
            for ref, part in zip((a1, a2, a3), split3(block)):
                ref[here] = part
            if i != j:
                for ref, part in zip((a1, a2, a3), split3(block.T)):
                    ref[here[1], here[0]] = part
    w_ref[rows:, :] = jnp.zeros((size - rows, outputs), jnp.float32)

    gr = lax.broadcasted_iota(jnp.int32, (outputs, outputs), 0)
    gc = lax.broadcasted_iota(jnp.int32, (outputs, outputs), 1)
    factor = total[slots[count - 1, count - 1]][offset:, offset:] / sample_total
    factor = jnp.where(gr == gc, factor + shift_g, factor)

    inverse_g = factor
    for k in range(outputs):
        row = inverse_g[k : k + 1, :]
        col = inverse_g[:, k : k + 1]
        inverse = 1.0 / inverse_g[k : k + 1, k : k + 1]
        scaled = row * inverse
        rest = inverse_g - col * scaled
        rest = jnp.where(gr == k, scaled, rest)
        rest = jnp.where(gc == k, -col * inverse, rest)
        inverse_g = jnp.where((gr == k) & (gc == k), inverse, rest)
    weights = w_ref[...]
    rhs = jnp.dot(
        weights, inverse_g, precision=lax.Precision.HIGHEST, preferred_element_type=jnp.float32
    )
    top = jnp.max(jnp.abs(rhs), axis=0, keepdims=True)
    top = jnp.where(top > 0.0, top, 1.0)
    residual = rhs / top
    x_ref[...] = jnp.zeros_like(x_ref)
    r_ref[...] = residual
    z = residual * inv_ref[...]
    p_ref[...] = z
    rz0 = jnp.sum(residual * z, axis=0, keepdims=True)
    goal = rz0 * 1e-13

    def unfinished(state):
        step, rz = state
        return (jnp.max(jnp.where(rz > goal, 1.0, 0.0)) > 0.0) & (step < 8 * size)

    def iterate(state):
        step, rz = state
        p = p_ref[...]
        for n, part in enumerate(split3(p)):
            pieces[:, n * outputs : (n + 1) * outputs] = part
        product = jnp.dot(a1[...], pieces[...], preferred_element_type=jnp.float32)
        second = jnp.dot(a2[...], pieces[:, : 2 * outputs], preferred_element_type=jnp.float32)
        third = jnp.dot(a3[...], pieces[:, :outputs], preferred_element_type=jnp.float32)
        q = (
            product[:, 2 * outputs :] + second[:, outputs:] + third
        ) + (product[:, outputs : 2 * outputs] + second[:, :outputs]) + product[:, :outputs]
        pq = jnp.sum(p * q, axis=0, keepdims=True)
        alpha = jnp.where(pq > 0.0, rz / jnp.where(pq > 0.0, pq, 1.0), 0.0)
        x_ref[...] += alpha * p
        left = r_ref[...] - alpha * q
        r_ref[...] = left
        preconditioned = left * inv_ref[...]
        after = jnp.sum(left * preconditioned, axis=0, keepdims=True)
        beta = jnp.where(rz > 0.0, after / jnp.where(rz > 0.0, rz, 1.0), 0.0)
        p_ref[...] = preconditioned + beta * p
        return step + 1, after

    lax.while_loop(unfinished, iterate, (jnp.int32(0), rz0))
    precond = x_ref[...] * top
    quadratic = jnp.sum(
        jnp.sum(precond * weights, axis=0, keepdims=True), axis=1, keepdims=True
    )
    clip = jnp.minimum(1.0, jnp.sqrt(trust_region_limit / (learning_rate**2 * quadratic)))
    flat_w = weights.T
    flat_u = (precond * clip).T
    for c in range(3):
        for b in range(3):
            for a in range(3):
                source = (c * 9 + b * 3 + a) * channels
                dest = (a * 9 + b * 3 + c) * channels
                weight_out[:, dest : dest + channels] = flat_w[:, source : source + channels]
                update_out[:, dest : dest + channels] = flat_u[:, source : source + channels]


MESH = pl.DeviceIdType.MESH


def bit_orders(dp, slab):
    core = [("dp", 1)] if dp > 1 else []
    along_y = [("dp", 1 << n) for n in range(1, dp.bit_length() - 1)]
    along_x = [("slab", 1)] if slab > 1 else []
    along_z = [("slab", 1 << n) for n in range(1, slab.bit_length() - 1)]
    groups = [along_x, along_y, along_z]
    return [core + groups[n] + groups[(n + 1) % 3] + groups[(n + 2) % 3] for n in range(3)]


def portion_plan(rows, orders):
    unit = rows // 14
    sizes = [5 * unit, 5 * unit, rows - 10 * unit]
    plan, start = [], 0
    for size, order in zip(sizes, orders):
        stages, length = [], size
        for bit in order:
            halves = length % 16 == 0
            length = length // 2 if halves else length
            stages.append((bit, length, halves))
        plan.append((start, size, stages))
        start += size
    return plan


def sum_kernel(plan, value, out, work, *scratch):
    stages = len(plan[0][2])
    recv = [scratch[n * stages : (n + 1) * stages] for n in range(len(plan))]
    send_sem, recv_sem = scratch[len(plan) * stages :]
    me = {"dp": lax.axis_index("dp"), "slab": lax.axis_index("slab")}

    def bit_of(bit):
        return (me[bit[0]] // bit[1]) % 2

    def partner(bit):
        there = dict(me)
        there[bit[0]] = me[bit[0]] + bit[1] * (1 - 2 * bit_of(bit))
        return (there["dp"], there["slab"])

    barrier = pltpu.get_barrier_semaphore()
    for bit, _, _ in plan[0][2]:
        pl.semaphore_signal(barrier, inc=1, device_id=partner(bit), device_id_type=MESH)
    pl.semaphore_wait(barrier, stages)

    first = [[start] for start, _, _ in plan]

    def window(start, length):
        return pl.ds(pl.multiple_of(start, 8), length)

    def begin(n, s):
        bit, length, halves = plan[n][2][s]
        before = first[n][s]
        mine = before + bit_of(bit) * length if halves else before
        other = before + (1 - bit_of(bit)) * length if halves else before
        first[n].append(mine)
        source = value if s == 0 else work
        copy = pltpu.make_async_remote_copy(
            src_ref=source.at[window(other, length)],
            dst_ref=recv[n][s],
            send_sem=send_sem.at[0, n, s],
            recv_sem=recv_sem.at[0, n, s],
            device_id=partner(bit),
            device_id_type=MESH,
        )
        copy.start()
        return copy

    flying = [begin(n, 0) for n in range(len(plan))]
    for s in range(stages):
        for n in range(len(plan)):
            _, length, _ = plan[n][2][s]
            flying[n].wait()
            here = window(first[n][s + 1], length)
            source = value if s == 0 else work
            target = work if s + 1 < stages else out
            target[here, :] = source[here, :] + recv[n][s][...]
            if s + 1 < stages:
                flying[n] = begin(n, s + 1)

    def spread(n, s):
        bit, length, _ = plan[n][2][s]
        here = window(first[n][s + 1], length)
        copy = pltpu.make_async_remote_copy(
            src_ref=out.at[here],
            dst_ref=out.at[here],
            send_sem=send_sem.at[1, n, s],
            recv_sem=recv_sem.at[1, n, s],
            device_id=partner(bit),
            device_id_type=MESH,
        )
        copy.start()
        return copy

    back = [[s for s in range(stages - 1, -1, -1) if stage[2][s][2]] for stage in plan]
    flying = [spread(n, back[n][0]) for n in range(len(plan))]
    for step in range(max(len(b) for b in back)):
        for n in range(len(plan)):
            if step < len(back[n]):
                flying[n].wait()
                if step + 1 < len(back[n]):
                    flying[n] = spread(n, back[n][step + 1])


def sum_everywhere(value):
    rows, lanes = value.shape
    plan = portion_plan(rows, bit_orders(lax.axis_size("dp"), lax.axis_size("slab")))
    stages = len(plan[0][2])
    buffers = [
        pltpu.VMEM((length, lanes), value.dtype) for _, _, steps in plan for _, length, _ in steps
    ]
    return pl.pallas_call(
        functools.partial(sum_kernel, plan),
        out_shape=jax.ShapeDtypeStruct(value.shape, value.dtype),
        in_specs=[pl.BlockSpec(memory_space=pltpu.VMEM)],
        out_specs=pl.BlockSpec(memory_space=pltpu.VMEM),
        scratch_shapes=[pltpu.VMEM(value.shape, value.dtype)]
        + buffers
        + [pltpu.SemaphoreType.DMA((2, len(plan), stages))] * 2,
        compiler_params=pltpu.CompilerParams(
            collective_id=0, has_side_effects=True, vmem_limit_bytes=24 * 1024 * 1024
        ),
        name="sum_everywhere",
    )(value)


def halo_kernel(size, parts, own, swapped, relayed, send_sem, recv_sem):
    dp, me = lax.axis_index("dp"), lax.axis_index("slab")
    odd = me % 2
    mate = me + 1 - 2 * odd
    target = me + 2 - 4 * odd
    source = me - 2 + 4 * odd
    gives = (target >= 0) & (target < size)
    takes = (source >= 0) & (source < size)
    barrier = pltpu.get_barrier_semaphore()
    pl.semaphore_signal(barrier, inc=1, device_id=(dp, mate), device_id_type=MESH)

    @pl.when(gives)
    def _():
        pl.semaphore_signal(barrier, inc=1, device_id=(dp, target), device_id_type=MESH)

    @pl.when(takes)
    def _():
        pl.semaphore_signal(barrier, inc=1, device_id=(dp, source), device_id_type=MESH)

    pl.semaphore_wait(barrier, 1 + gives.astype(jnp.int32) + takes.astype(jnp.int32))
    step = own.shape[1] // parts

    def piece(kind, n):
        here = slice(n * step, (n + 1) * step)
        return pltpu.make_async_remote_copy(
            src_ref=(own if kind == 0 else swapped).at[:, here],
            dst_ref=(swapped if kind == 0 else relayed).at[:, here],
            send_sem=send_sem.at[kind, n],
            recv_sem=recv_sem.at[kind, n],
            device_id=(dp, mate if kind == 0 else target),
            device_id_type=MESH,
        )

    for n in range(parts):
        piece(0, n).start()

    @pl.when(jnp.logical_not(takes))
    def _():
        relayed[...] = jnp.zeros_like(relayed)

    for n in range(parts):
        piece(0, n).wait_recv()

        @pl.when(gives)
        def _():
            piece(1, n).start()

    for n in range(parts):
        piece(0, n).wait_send()

        @pl.when(gives)
        def _():
            piece(1, n).wait_send()

        @pl.when(takes)
        def _():
            piece(1, n).wait_recv()


def halo(plane):
    size, parts = lax.axis_size("slab"), 8
    swapped, relayed = pl.pallas_call(
        functools.partial(halo_kernel, size, parts),
        out_shape=[jax.ShapeDtypeStruct(plane.shape, plane.dtype)] * 2,
        in_specs=[pl.BlockSpec(memory_space=pltpu.VMEM)],
        out_specs=[pl.BlockSpec(memory_space=pltpu.VMEM)] * 2,
        scratch_shapes=[pltpu.SemaphoreType.DMA((2, parts))] * 2,
        compiler_params=pltpu.CompilerParams(
            collective_id=1, has_side_effects=True, vmem_limit_bytes=16 * 1024 * 1024
        ),
        name="halo",
    )(plane)
    return swapped, relayed


def shards(acts, grads, picks):
    volumes, channels, planes, height, width = acts.shape
    outputs = grads.shape[1]
    cells = height * width
    own = acts.reshape(channels, cells)
    rows = grads.reshape(outputs, cells)
    swapped, relayed = halo(own)
    samples = picks.shape[1]
    chunks = cells // CHUNK
    position = jnp.arange(samples, dtype=jnp.int32) * 32 + picks.reshape(samples)
    column = position % width
    targets = jnp.stack(
        [
            jnp.where((column + d >= 0) & (column + d < width), position + d, -1)
            for d in (-1, 0, 1)
        ]
    )
    targets = targets.reshape(3, chunks, samples // chunks).transpose(0, 2, 1)
    targets = targets.reshape(3 * (samples // chunks), chunks)
    size = 27 * channels + outputs
    count = size // BLOCK
    blocks = count * (count + 1) // 2
    partial = pl.pallas_call(
        functools.partial(local_kernel, width),
        out_shape=jax.ShapeDtypeStruct((blocks, BLOCK, BLOCK), jnp.float32),
        in_specs=[pl.BlockSpec(memory_space=pltpu.VMEM)] * 5,
        out_specs=pl.BlockSpec(memory_space=pltpu.VMEM),
        scratch_shapes=[
            pltpu.VMEM((3 * channels, cells + 2 * width), jnp.bfloat16),
            pltpu.VMEM((size, samples), jnp.float32),
            pltpu.VMEM((size, BLOCK), jnp.float32),
        ],
        compiler_params=pltpu.CompilerParams(vmem_limit_bytes=48 * 1024 * 1024),
        name="local_sums",
    )(own, swapped, relayed, rows, targets)
    total = sum_everywhere(partial.reshape(-1, BLOCK)).reshape(partial.shape)
    everyone = lax.axis_size("dp") * lax.axis_size("slab") * volumes
    return pl.pallas_call(
        functools.partial(
            solve_kernel, everyone * planes * cells, everyone * samples, channels, outputs
        ),
        out_shape=[jax.ShapeDtypeStruct((outputs, 27 * channels), jnp.float32)] * 2,
        in_specs=[pl.BlockSpec(memory_space=pltpu.VMEM)],
        out_specs=[pl.BlockSpec(memory_space=pltpu.VMEM)] * 2,
        scratch_shapes=[pltpu.VMEM((size, size), jnp.bfloat16)] * 3
        + [pltpu.VMEM((size, 3 * outputs), jnp.bfloat16)]
        + [pltpu.VMEM((size, outputs), jnp.float32)] * 4
        + [pltpu.VMEM((size, 1), jnp.float32)],
        compiler_params=pltpu.CompilerParams(vmem_limit_bytes=48 * 1024 * 1024),
        name="solve",
    )(total)


def solution(mesh):
    return jax.shard_map(
        shards,
        mesh=mesh,
        in_specs=(
            P("dp", None, "slab", None, None),
            P("dp", None, "slab", None, None),
            P("dp", "slab"),
        ),
        out_specs=(P(), P()),
        check_vma=False,
    )
```

```python
import functools
import math

import jax
import jax.numpy as jnp
from jax import lax
from jax.experimental import pallas as pl
from jax.experimental.pallas import tpu as pltpu
from jax.sharding import PartitionSpec as P

epsilon = 1e-06
damping = 0.1
trust_region_limit = 0.3
learning_rate = 0.01
BLOCK = 128
CHUNK = 1024
NT = (((1,), (1,)), ((), ()))


def local_kernel(width, own, swapped, relayed, grads, targets, out, apad, samples, wsum):
    channels, cells = own.shape
    outputs = grads.shape[0]
    per_chunk = targets.shape[0] // 3
    rows = 27 * channels
    total = samples.shape[0]
    third = 9 * channels
    odd = lax.axis_index("slab") % 2 == 1
    inner = slice(width, width + cells)
    apad[channels : 2 * channels, inner] = own[...]

    @pl.when(odd)
    def _():
        apad[:channels, inner] = swapped[...]
        apad[2 * channels :, inner] = relayed[...]

    @pl.when(jnp.logical_not(odd))
    def _():
        apad[:channels, inner] = relayed[...]
        apad[2 * channels :, inner] = swapped[...]

    apad[:, 0:width] = jnp.zeros((3 * channels, width), apad.dtype)
    apad[:, width + cells :] = jnp.zeros((3 * channels, width), apad.dtype)
    lane = lax.broadcasted_iota(jnp.int32, (outputs, CHUNK), 1) % width
    position = lax.broadcasted_iota(jnp.int32, (3 * per_chunk, CHUNK), 1)
    sums = jnp.zeros((third, 3 * outputs), jnp.float32)
    for k in range(cells // CHUNK):
        base = k * CHUNK
        g = grads[:, base : base + CHUNK]
        wide = g.astype(jnp.float32)
        left = jnp.where(lane == width - 1, 0.0, pltpu.roll(wide, CHUNK - 1, 1)).astype(g.dtype)
        right = jnp.where(lane == 0, 0.0, pltpu.roll(wide, 1, 1)).astype(g.dtype)
        select = jnp.where(position == targets[:, k : k + 1] - base, 1.0, 0.0).astype(g.dtype)
        lhs = jnp.concatenate(
            [apad[:, base + b * width : base + b * width + CHUNK] for b in range(3)] + [g], axis=0
        )
        rhs = jnp.concatenate([left, g, right, select], axis=0)
        both = lax.dot_general(lhs, rhs, NT, preferred_element_type=jnp.float32)
        sums += both[:third, : 3 * outputs]
        where = slice(k * per_chunk, (k + 1) * per_chunk)
        for c in range(3):
            start = 3 * outputs + c * per_chunk
            samples[c * third : (c + 1) * third, where] = both[:third, start : start + per_chunk]
        start = 3 * outputs + per_chunk
        samples[rows : rows + outputs, where] = both[third:, start : start + per_chunk]
    offset = BLOCK - outputs
    for c in range(3):
        wsum[c * third : (c + 1) * third, offset:] = sums[:, c * outputs : (c + 1) * outputs]
    count = total // BLOCK
    r = lax.broadcasted_iota(jnp.int32, (BLOCK, BLOCK), 0)
    l = lax.broadcasted_iota(jnp.int32, (BLOCK, BLOCK), 1)
    vectors = samples[...].astype(jnp.bfloat16)
    slot = 0
    for i in range(count):
        gram = lax.dot_general(
            vectors[i * BLOCK : (i + 1) * BLOCK],
            vectors[i * BLOCK :],
            NT,
            preferred_element_type=jnp.float32,
        )
        for j in range(i, count):
            block = gram[:, (j - i) * BLOCK : (j - i + 1) * BLOCK]
            if j == count - 1:
                weights = wsum[i * BLOCK : (i + 1) * BLOCK, :]
                block = jnp.where((l >= offset) & (r + i * BLOCK < rows), weights, block)
            out[slot] = block
            slot += 1


def split3(value):
    first = value.astype(jnp.bfloat16)
    rest = value - first.astype(jnp.float32)
    second = rest.astype(jnp.bfloat16)
    third = (rest - second.astype(jnp.float32)).astype(jnp.bfloat16)
    return first, second, third


def solve_kernel(
    positions, sample_total, channels, outputs, total, weight_out, update_out,
    a1, a2, a3, pieces, x_ref, r_ref, p_ref, w_ref, inv_ref
):
    rows = 27 * channels
    size = a1.shape[0]
    count = size // BLOCK
    offset = BLOCK - outputs
    r = lax.broadcasted_iota(jnp.int32, (BLOCK, BLOCK), 0)
    l = lax.broadcasted_iota(jnp.int32, (BLOCK, BLOCK), 1)
    slots = {}
    for i in range(count):
        for j in range(i, count):
            slots[i, j] = len(slots)
    diagonals = [
        jnp.sum(jnp.where(r == l, total[slots[i, i]], 0.0), axis=1, keepdims=True)
        for i in range(count)
    ]
    column = lax.broadcasted_iota(jnp.int32, (BLOCK, 1), 0)
    trace_a = jnp.zeros((1, 1), jnp.float32)
    trace_g = jnp.zeros((1, 1), jnp.float32)
    for i in range(count):
        inside = column + i * BLOCK < rows
        trace_a += jnp.sum(jnp.where(inside, diagonals[i], 0.0), axis=0, keepdims=True)
        trace_g += jnp.sum(jnp.where(inside, 0.0, diagonals[i]), axis=0, keepdims=True)
    ratio = jnp.sqrt(
        (trace_a / sample_total / rows + epsilon) / (trace_g / sample_total / outputs + epsilon)
    )
    shift_a = ratio * math.sqrt(damping)
    shift_g = math.sqrt(damping) / ratio
    for i in range(count):
        inside = column + i * BLOCK < rows
        inv_ref[i * BLOCK : (i + 1) * BLOCK, :] = 1.0 / jnp.where(
            inside, diagonals[i] / sample_total + shift_a, 1.0
        )
        for j in range(i, count):
            block = total[slots[i, j]] / sample_total
            if j == count - 1:
                w_ref[i * BLOCK : (i + 1) * BLOCK, :] = (
                    total[slots[i, j]][:, offset:] / math.sqrt(positions)
                )
                block = jnp.where((r + i * BLOCK < rows) & (l + j * BLOCK < rows), block, 0.0)
            if i == j:
                shift = jnp.where(r + i * BLOCK < rows, shift_a, 1.0)
                block = jnp.where(r == l, block + shift, block)
            here = (slice(i * BLOCK, (i + 1) * BLOCK), slice(j * BLOCK, (j + 1) * BLOCK))
            for ref, part in zip((a1, a2, a3), split3(block)):
                ref[here] = part
            if i != j:
                for ref, part in zip((a1, a2, a3), split3(block.T)):
                    ref[here[1], here[0]] = part
    w_ref[rows:, :] = jnp.zeros((size - rows, outputs), jnp.float32)

    gr = lax.broadcasted_iota(jnp.int32, (outputs, outputs), 0)
    gc = lax.broadcasted_iota(jnp.int32, (outputs, outputs), 1)
    factor = total[slots[count - 1, count - 1]][offset:, offset:] / sample_total
    factor = jnp.where(gr == gc, factor + shift_g, factor)

    inverse_g = factor
    for k in range(outputs):
        row = inverse_g[k : k + 1, :]
        col = inverse_g[:, k : k + 1]
        inverse = 1.0 / inverse_g[k : k + 1, k : k + 1]
        scaled = row * inverse
        rest = inverse_g - col * scaled
        rest = jnp.where(gr == k, scaled, rest)
        rest = jnp.where(gc == k, -col * inverse, rest)
        inverse_g = jnp.where((gr == k) & (gc == k), inverse, rest)
    weights = w_ref[...]
    rhs = jnp.dot(
        weights, inverse_g, precision=lax.Precision.HIGHEST, preferred_element_type=jnp.float32
    )
    top = jnp.max(jnp.abs(rhs), axis=0, keepdims=True)
    top = jnp.where(top > 0.0, top, 1.0)
    residual = rhs / top
    x_ref[...] = jnp.zeros_like(x_ref)
    r_ref[...] = residual
    z = residual * inv_ref[...]
    p_ref[...] = z
    rz0 = jnp.sum(residual * z, axis=0, keepdims=True)
    goal = rz0 * 1e-13

    def unfinished(state):
        step, rz = state
        return (jnp.max(jnp.where(rz > goal, 1.0, 0.0)) > 0.0) & (step < 8 * size)

    def iterate(state):
        step, rz = state
        p = p_ref[...]
        for n, part in enumerate(split3(p)):
            pieces[:, n * outputs : (n + 1) * outputs] = part
        product = jnp.dot(a1[...], pieces[...], preferred_element_type=jnp.float32)
        second = jnp.dot(a2[...], pieces[:, : 2 * outputs], preferred_element_type=jnp.float32)
        third = jnp.dot(a3[...], pieces[:, :outputs], preferred_element_type=jnp.float32)
        q = (
            product[:, 2 * outputs :] + second[:, outputs:] + third
        ) + (product[:, outputs : 2 * outputs] + second[:, :outputs]) + product[:, :outputs]
        pq = jnp.sum(p * q, axis=0, keepdims=True)
        alpha = jnp.where(pq > 0.0, rz / jnp.where(pq > 0.0, pq, 1.0), 0.0)
        x_ref[...] += alpha * p
        left = r_ref[...] - alpha * q
        r_ref[...] = left
        preconditioned = left * inv_ref[...]
        after = jnp.sum(left * preconditioned, axis=0, keepdims=True)
        beta = jnp.where(rz > 0.0, after / jnp.where(rz > 0.0, rz, 1.0), 0.0)
        p_ref[...] = preconditioned + beta * p
        return step + 1, after

    lax.while_loop(unfinished, iterate, (jnp.int32(0), rz0))
    precond = x_ref[...] * top
    quadratic = jnp.sum(
        jnp.sum(precond * weights, axis=0, keepdims=True), axis=1, keepdims=True
    )
    clip = jnp.minimum(1.0, jnp.sqrt(trust_region_limit / (learning_rate**2 * quadratic)))
    flat_w = weights.T
    flat_u = (precond * clip).T
    for c in range(3):
        for b in range(3):
            for a in range(3):
                source = (c * 9 + b * 3 + a) * channels
                dest = (a * 9 + b * 3 + c) * channels
                weight_out[:, dest : dest + channels] = flat_w[:, source : source + channels]
                update_out[:, dest : dest + channels] = flat_u[:, source : source + channels]


MESH = pl.DeviceIdType.MESH


def bit_orders(dp, slab):
    core = [("dp", 1)] if dp > 1 else []
    along_y = [("dp", 1 << n) for n in range(1, dp.bit_length() - 1)]
    along_x = [("slab", 1)] if slab > 1 else []
    along_z = [("slab", 1 << n) for n in range(1, slab.bit_length() - 1)]
    groups = [along_x, along_y, along_z]
    return [core + groups[n] + groups[(n + 1) % 3] + groups[(n + 2) % 3] for n in range(3)]


def portion_plan(rows, orders):
    unit = rows // 14
    sizes = [3 * unit, 3 * unit, 2 * unit, 2 * unit, 2 * unit, rows - 12 * unit]
    orders = orders + orders
    plan, start = [], 0
    for size, order in zip(sizes, orders):
        stages, length = [], size
        for bit in order:
            halves = length % 16 == 0
            length = length // 2 if halves else length
            stages.append((bit, length, halves))
        plan.append((start, size, stages))
        start += size
    return plan


def sum_kernel(plan, value, out, work, *scratch):
    stages = len(plan[0][2])
    recv = [scratch[n * stages : (n + 1) * stages] for n in range(len(plan))]
    send_sem, recv_sem = scratch[len(plan) * stages :]
    me = {"dp": lax.axis_index("dp"), "slab": lax.axis_index("slab")}

    def bit_of(bit):
        return (me[bit[0]] // bit[1]) % 2

    def partner(bit):
        there = dict(me)
        there[bit[0]] = me[bit[0]] + bit[1] * (1 - 2 * bit_of(bit))
        return (there["dp"], there["slab"])

    barrier = pltpu.get_barrier_semaphore()
    for bit, _, _ in plan[0][2]:
        pl.semaphore_signal(barrier, inc=1, device_id=partner(bit), device_id_type=MESH)
    pl.semaphore_wait(barrier, stages)

    first = [[start] for start, _, _ in plan]

    def window(start, length):
        return pl.ds(pl.multiple_of(start, 8), length)

    def begin(n, s):
        bit, length, halves = plan[n][2][s]
        before = first[n][s]
        mine = before + bit_of(bit) * length if halves else before
        other = before + (1 - bit_of(bit)) * length if halves else before
        first[n].append(mine)
        source = value if s == 0 else work
        copy = pltpu.make_async_remote_copy(
            src_ref=source.at[window(other, length)],
            dst_ref=recv[n][s],
            send_sem=send_sem.at[0, n, s],
            recv_sem=recv_sem.at[0, n, s],
            device_id=partner(bit),
            device_id_type=MESH,
        )
        copy.start()
        return copy

    flying = [begin(n, 0) for n in range(len(plan))]
    for s in range(stages):
        for n in range(len(plan)):
            _, length, _ = plan[n][2][s]
            flying[n].wait()
            here = window(first[n][s + 1], length)
            source = value if s == 0 else work
            target = work if s + 1 < stages else out
            target[here, :] = source[here, :] + recv[n][s][...]
            if s + 1 < stages:
                flying[n] = begin(n, s + 1)

    def spread(n, s):
        bit, length, _ = plan[n][2][s]
        here = window(first[n][s + 1], length)
        copy = pltpu.make_async_remote_copy(
            src_ref=out.at[here],
            dst_ref=out.at[here],
            send_sem=send_sem.at[1, n, s],
            recv_sem=recv_sem.at[1, n, s],
            device_id=partner(bit),
            device_id_type=MESH,
        )
        copy.start()
        return copy

    back = [[s for s in range(stages - 1, -1, -1) if stage[2][s][2]] for stage in plan]
    flying = [spread(n, back[n][0]) for n in range(len(plan))]
    for step in range(max(len(b) for b in back)):
        for n in range(len(plan)):
            if step < len(back[n]):
                flying[n].wait()
                if step + 1 < len(back[n]):
                    flying[n] = spread(n, back[n][step + 1])


def sum_everywhere(value):
    rows, lanes = value.shape
    plan = portion_plan(rows, bit_orders(lax.axis_size("dp"), lax.axis_size("slab")))
    stages = len(plan[0][2])
    buffers = [
        pltpu.VMEM((length, lanes), value.dtype) for _, _, steps in plan for _, length, _ in steps
    ]
    return pl.pallas_call(
        functools.partial(sum_kernel, plan),
        out_shape=jax.ShapeDtypeStruct(value.shape, value.dtype),
        in_specs=[pl.BlockSpec(memory_space=pltpu.VMEM)],
        out_specs=pl.BlockSpec(memory_space=pltpu.VMEM),
        scratch_shapes=[pltpu.VMEM(value.shape, value.dtype)]
        + buffers
        + [pltpu.SemaphoreType.DMA((2, len(plan), stages))] * 2,
        compiler_params=pltpu.CompilerParams(
            collective_id=0, has_side_effects=True, vmem_limit_bytes=24 * 1024 * 1024
        ),
        name="sum_everywhere",
    )(value)


def halo_kernel(size, parts, own, swapped, relayed, send_sem, recv_sem):
    dp, me = lax.axis_index("dp"), lax.axis_index("slab")
    odd = me % 2
    mate = me + 1 - 2 * odd
    target = me + 2 - 4 * odd
    source = me - 2 + 4 * odd
    gives = (target >= 0) & (target < size)
    takes = (source >= 0) & (source < size)
    barrier = pltpu.get_barrier_semaphore()
    pl.semaphore_signal(barrier, inc=1, device_id=(dp, mate), device_id_type=MESH)

    @pl.when(gives)
    def _():
        pl.semaphore_signal(barrier, inc=1, device_id=(dp, target), device_id_type=MESH)

    @pl.when(takes)
    def _():
        pl.semaphore_signal(barrier, inc=1, device_id=(dp, source), device_id_type=MESH)

    pl.semaphore_wait(barrier, 1 + gives.astype(jnp.int32) + takes.astype(jnp.int32))
    step = own.shape[1] // parts

    def piece(kind, n):
        here = slice(n * step, (n + 1) * step)
        return pltpu.make_async_remote_copy(
            src_ref=(own if kind == 0 else swapped).at[:, here],
            dst_ref=(swapped if kind == 0 else relayed).at[:, here],
            send_sem=send_sem.at[kind, n],
            recv_sem=recv_sem.at[kind, n],
            device_id=(dp, mate if kind == 0 else target),
            device_id_type=MESH,
        )

    for n in range(parts):
        piece(0, n).start()

    @pl.when(jnp.logical_not(takes))
    def _():
        relayed[...] = jnp.zeros_like(relayed)

    for n in range(parts):
        piece(0, n).wait_recv()

        @pl.when(gives)
        def _():
            piece(1, n).start()

    for n in range(parts):
        piece(0, n).wait_send()

        @pl.when(gives)
        def _():
            piece(1, n).wait_send()

        @pl.when(takes)
        def _():
            piece(1, n).wait_recv()


def halo(plane):
    size, parts = lax.axis_size("slab"), 8
    swapped, relayed = pl.pallas_call(
        functools.partial(halo_kernel, size, parts),
        out_shape=[jax.ShapeDtypeStruct(plane.shape, plane.dtype)] * 2,
        in_specs=[pl.BlockSpec(memory_space=pltpu.VMEM)],
        out_specs=[pl.BlockSpec(memory_space=pltpu.VMEM)] * 2,
        scratch_shapes=[pltpu.SemaphoreType.DMA((2, parts))] * 2,
        compiler_params=pltpu.CompilerParams(
            collective_id=1, has_side_effects=True, vmem_limit_bytes=16 * 1024 * 1024
        ),
        name="halo",
    )(plane)
    return swapped, relayed


def shards(acts, grads, picks):
    volumes, channels, planes, height, width = acts.shape
    outputs = grads.shape[1]
    cells = height * width
    own = acts.reshape(channels, cells)
    rows = grads.reshape(outputs, cells)
    swapped, relayed = halo(own)
    samples = picks.shape[1]
    chunks = cells // CHUNK
    position = jnp.arange(samples, dtype=jnp.int32) * 32 + picks.reshape(samples)
    column = position % width
    targets = jnp.stack(
        [
            jnp.where((column + d >= 0) & (column + d < width), position + d, -1)
            for d in (-1, 0, 1)
        ]
    )
    targets = targets.reshape(3, chunks, samples // chunks).transpose(0, 2, 1)
    targets = targets.reshape(3 * (samples // chunks), chunks)
    size = 27 * channels + outputs
    count = size // BLOCK
    blocks = count * (count + 1) // 2
    partial = pl.pallas_call(
        functools.partial(local_kernel, width),
        out_shape=jax.ShapeDtypeStruct((blocks, BLOCK, BLOCK), jnp.float32),
        in_specs=[pl.BlockSpec(memory_space=pltpu.VMEM)] * 5,
        out_specs=pl.BlockSpec(memory_space=pltpu.VMEM),
        scratch_shapes=[
            pltpu.VMEM((3 * channels, cells + 2 * width), jnp.bfloat16),
            pltpu.VMEM((size, samples), jnp.float32),
            pltpu.VMEM((size, BLOCK), jnp.float32),
        ],
        compiler_params=pltpu.CompilerParams(vmem_limit_bytes=48 * 1024 * 1024),
        name="local_sums",
    )(own, swapped, relayed, rows, targets)
    total = sum_everywhere(partial.reshape(-1, BLOCK)).reshape(partial.shape)
    everyone = lax.axis_size("dp") * lax.axis_size("slab") * volumes
    return pl.pallas_call(
        functools.partial(
            solve_kernel, everyone * planes * cells, everyone * samples, channels, outputs
        ),
        out_shape=[jax.ShapeDtypeStruct((outputs, 27 * channels), jnp.float32)] * 2,
        in_specs=[pl.BlockSpec(memory_space=pltpu.VMEM)],
        out_specs=[pl.BlockSpec(memory_space=pltpu.VMEM)] * 2,
        scratch_shapes=[pltpu.VMEM((size, size), jnp.bfloat16)] * 3
        + [pltpu.VMEM((size, 3 * outputs), jnp.bfloat16)]
        + [pltpu.VMEM((size, outputs), jnp.float32)] * 4
        + [pltpu.VMEM((size, 1), jnp.float32)],
        compiler_params=pltpu.CompilerParams(vmem_limit_bytes=48 * 1024 * 1024),
        name="solve",
    )(total)


def solution(mesh):
    return jax.shard_map(
        shards,
        mesh=mesh,
        in_specs=(
            P("dp", None, "slab", None, None),
            P("dp", None, "slab", None, None),
            P("dp", "slab"),
        ),
        out_specs=(P(), P()),
        check_vma=False,
    )
```

```python
import functools
import math

import jax
import jax.numpy as jnp
from jax import lax
from jax.experimental import pallas as pl
from jax.experimental.pallas import tpu as pltpu
from jax.sharding import PartitionSpec as P

epsilon = 1e-06
damping = 0.1
trust_region_limit = 0.3
learning_rate = 0.01
BLOCK = 128
CHUNK = 1024
NT = (((1,), (1,)), ((), ()))


def local_kernel(width, own, swapped, relayed, grads, targets, out, apad, samples, wsum):
    channels, cells = own.shape
    outputs = grads.shape[0]
    per_chunk = targets.shape[0] // 3
    rows = 27 * channels
    total = samples.shape[0]
    third = 9 * channels
    odd = lax.axis_index("slab") % 2 == 1
    inner = slice(width, width + cells)
    apad[channels : 2 * channels, inner] = own[...]

    @pl.when(odd)
    def _():
        apad[:channels, inner] = swapped[...]
        apad[2 * channels :, inner] = relayed[...]

    @pl.when(jnp.logical_not(odd))
    def _():
        apad[:channels, inner] = relayed[...]
        apad[2 * channels :, inner] = swapped[...]

    apad[:, 0:width] = jnp.zeros((3 * channels, width), apad.dtype)
    apad[:, width + cells :] = jnp.zeros((3 * channels, width), apad.dtype)
    lane = lax.broadcasted_iota(jnp.int32, (outputs, CHUNK), 1) % width
    position = lax.broadcasted_iota(jnp.int32, (3 * per_chunk, CHUNK), 1)
    sums = jnp.zeros((third, 3 * outputs), jnp.float32)
    for k in range(cells // CHUNK):
        base = k * CHUNK
        g = grads[:, base : base + CHUNK]
        wide = g.astype(jnp.float32)
        left = jnp.where(lane == width - 1, 0.0, pltpu.roll(wide, CHUNK - 1, 1)).astype(g.dtype)
        right = jnp.where(lane == 0, 0.0, pltpu.roll(wide, 1, 1)).astype(g.dtype)
        select = jnp.where(position == targets[:, k : k + 1] - base, 1.0, 0.0).astype(g.dtype)
        lhs = jnp.concatenate(
            [apad[:, base + b * width : base + b * width + CHUNK] for b in range(3)] + [g], axis=0
        )
        rhs = jnp.concatenate([left, g, right, select], axis=0)
        both = lax.dot_general(lhs, rhs, NT, preferred_element_type=jnp.float32)
        sums += both[:third, : 3 * outputs]
        where = slice(k * per_chunk, (k + 1) * per_chunk)
        for c in range(3):
            start = 3 * outputs + c * per_chunk
            samples[c * third : (c + 1) * third, where] = both[:third, start : start + per_chunk]
        start = 3 * outputs + per_chunk
        samples[rows : rows + outputs, where] = both[third:, start : start + per_chunk]
    offset = BLOCK - outputs
    for c in range(3):
        wsum[c * third : (c + 1) * third, offset:] = sums[:, c * outputs : (c + 1) * outputs]
    count = total // BLOCK
    r = lax.broadcasted_iota(jnp.int32, (BLOCK, BLOCK), 0)
    l = lax.broadcasted_iota(jnp.int32, (BLOCK, BLOCK), 1)
    vectors = samples[...].astype(jnp.bfloat16)
    slot = 0
    for i in range(count):
        gram = lax.dot_general(
            vectors[i * BLOCK : (i + 1) * BLOCK],
            vectors[i * BLOCK :],
            NT,
            preferred_element_type=jnp.float32,
        )
        for j in range(i, count):
            block = gram[:, (j - i) * BLOCK : (j - i + 1) * BLOCK]
            if j == count - 1:
                weights = wsum[i * BLOCK : (i + 1) * BLOCK, :]
                block = jnp.where((l >= offset) & (r + i * BLOCK < rows), weights, block)
            out[slot] = block
            slot += 1


def split3(value):
    first = value.astype(jnp.bfloat16)
    rest = value - first.astype(jnp.float32)
    second = rest.astype(jnp.bfloat16)
    third = (rest - second.astype(jnp.float32)).astype(jnp.bfloat16)
    return first, second, third


def solve_kernel(
    positions, sample_total, channels, outputs, total, weight_out, update_out,
    a1, a2, a3, pieces, x_ref, r_ref, p_ref, w_ref, inv_ref
):
    rows = 27 * channels
    size = a1.shape[0]
    count = size // BLOCK
    offset = BLOCK - outputs
    r = lax.broadcasted_iota(jnp.int32, (BLOCK, BLOCK), 0)
    l = lax.broadcasted_iota(jnp.int32, (BLOCK, BLOCK), 1)
    slots = {}
    for i in range(count):
        for j in range(i, count):
            slots[i, j] = len(slots)
    diagonals = [
        jnp.sum(jnp.where(r == l, total[slots[i, i]], 0.0), axis=1, keepdims=True)
        for i in range(count)
    ]
    column = lax.broadcasted_iota(jnp.int32, (BLOCK, 1), 0)
    trace_a = jnp.zeros((1, 1), jnp.float32)
    trace_g = jnp.zeros((1, 1), jnp.float32)
    for i in range(count):
        inside = column + i * BLOCK < rows
        trace_a += jnp.sum(jnp.where(inside, diagonals[i], 0.0), axis=0, keepdims=True)
        trace_g += jnp.sum(jnp.where(inside, 0.0, diagonals[i]), axis=0, keepdims=True)
    ratio = jnp.sqrt(
        (trace_a / sample_total / rows + epsilon) / (trace_g / sample_total / outputs + epsilon)
    )
    shift_a = ratio * math.sqrt(damping)
    shift_g = math.sqrt(damping) / ratio
    for i in range(count):
        inside = column + i * BLOCK < rows
        inv_ref[i * BLOCK : (i + 1) * BLOCK, :] = 1.0 / jnp.where(
            inside, diagonals[i] / sample_total + shift_a, 1.0
        )
        for j in range(i, count):
            block = total[slots[i, j]] / sample_total
            if j == count - 1:
                w_ref[i * BLOCK : (i + 1) * BLOCK, :] = (
                    total[slots[i, j]][:, offset:] / math.sqrt(positions)
                )
                block = jnp.where((r + i * BLOCK < rows) & (l + j * BLOCK < rows), block, 0.0)
            if i == j:
                shift = jnp.where(r + i * BLOCK < rows, shift_a, 1.0)
                block = jnp.where(r == l, block + shift, block)
            here = (slice(i * BLOCK, (i + 1) * BLOCK), slice(j * BLOCK, (j + 1) * BLOCK))
            for ref, part in zip((a1, a2, a3), split3(block)):
                ref[here] = part
            if i != j:
                for ref, part in zip((a1, a2, a3), split3(block.T)):
                    ref[here[1], here[0]] = part
    w_ref[rows:, :] = jnp.zeros((size - rows, outputs), jnp.float32)

    gr = lax.broadcasted_iota(jnp.int32, (outputs, outputs), 0)
    gc = lax.broadcasted_iota(jnp.int32, (outputs, outputs), 1)
    factor = total[slots[count - 1, count - 1]][offset:, offset:] / sample_total
    factor = jnp.where(gr == gc, factor + shift_g, factor)

    inverse_g = factor
    for k in range(outputs):
        row = inverse_g[k : k + 1, :]
        col = inverse_g[:, k : k + 1]
        inverse = 1.0 / inverse_g[k : k + 1, k : k + 1]
        scaled = row * inverse
        rest = inverse_g - col * scaled
        rest = jnp.where(gr == k, scaled, rest)
        rest = jnp.where(gc == k, -col * inverse, rest)
        inverse_g = jnp.where((gr == k) & (gc == k), inverse, rest)
    weights = w_ref[...]
    rhs = jnp.dot(
        weights, inverse_g, precision=lax.Precision.HIGHEST, preferred_element_type=jnp.float32
    )
    top = jnp.max(jnp.abs(rhs), axis=0, keepdims=True)
    top = jnp.where(top > 0.0, top, 1.0)
    residual = rhs / top
    x_ref[...] = jnp.zeros_like(x_ref)
    r_ref[...] = residual
    z = residual * inv_ref[...]
    p_ref[...] = z
    rz0 = jnp.sum(residual * z, axis=0, keepdims=True)
    goal = rz0 * 1e-13

    def unfinished(state):
        step, rz = state
        return (jnp.max(jnp.where(rz > goal, 1.0, 0.0)) > 0.0) & (step < 8 * size)

    def iterate(state):
        step, rz = state
        p = p_ref[...]
        for n, part in enumerate(split3(p)):
            pieces[:, n * outputs : (n + 1) * outputs] = part
        product = jnp.dot(a1[...], pieces[...], preferred_element_type=jnp.float32)
        second = jnp.dot(a2[...], pieces[:, : 2 * outputs], preferred_element_type=jnp.float32)
        third = jnp.dot(a3[...], pieces[:, :outputs], preferred_element_type=jnp.float32)
        q = (
            product[:, 2 * outputs :] + second[:, outputs:] + third
        ) + (product[:, outputs : 2 * outputs] + second[:, :outputs]) + product[:, :outputs]
        pq = jnp.sum(p * q, axis=0, keepdims=True)
        alpha = jnp.where(pq > 0.0, rz / jnp.where(pq > 0.0, pq, 1.0), 0.0)
        x_ref[...] += alpha * p
        left = r_ref[...] - alpha * q
        r_ref[...] = left
        preconditioned = left * inv_ref[...]
        after = jnp.sum(left * preconditioned, axis=0, keepdims=True)
        beta = jnp.where(rz > 0.0, after / jnp.where(rz > 0.0, rz, 1.0), 0.0)
        p_ref[...] = preconditioned + beta * p
        return step + 1, after

    lax.while_loop(unfinished, iterate, (jnp.int32(0), rz0))
    precond = x_ref[...] * top
    quadratic = jnp.sum(
        jnp.sum(precond * weights, axis=0, keepdims=True), axis=1, keepdims=True
    )
    clip = jnp.minimum(1.0, jnp.sqrt(trust_region_limit / (learning_rate**2 * quadratic)))
    flat_w = weights.T
    flat_u = (precond * clip).T
    for c in range(3):
        for b in range(3):
            for a in range(3):
                source = (c * 9 + b * 3 + a) * channels
                dest = (a * 9 + b * 3 + c) * channels
                weight_out[:, dest : dest + channels] = flat_w[:, source : source + channels]
                update_out[:, dest : dest + channels] = flat_u[:, source : source + channels]


MESH = pl.DeviceIdType.MESH


def bit_orders(dp, slab):
    core = [("dp", 1)] if dp > 1 else []
    along_y = [("dp", 1 << n) for n in range(1, dp.bit_length() - 1)]
    along_x = [("slab", 1)] if slab > 1 else []
    along_z = [("slab", 1 << n) for n in range(1, slab.bit_length() - 1)]
    groups = [along_x, along_y, along_z]
    return [core + groups[n] + groups[(n + 1) % 3] + groups[(n + 2) % 3] for n in range(3)]


def portion_plan(rows, orders):
    unit = rows // 14
    sizes = [3 * unit, 3 * unit, 2 * unit, 2 * unit, 2 * unit, rows - 12 * unit]
    orders = orders + orders
    plan, start = [], 0
    for size, order in zip(sizes, orders):
        stages, length = [], size
        for bit in order:
            halves = length % 16 == 0
            length = length // 2 if halves else length
            stages.append((bit, length, halves))
        plan.append((start, size, stages))
        start += size
    return plan


def sum_kernel(plan, value, out, work, *scratch):
    stages = len(plan[0][2])
    recv = [scratch[n * stages : (n + 1) * stages] for n in range(len(plan))]
    send_sem, recv_sem = scratch[len(plan) * stages :]
    me = {"dp": lax.axis_index("dp"), "slab": lax.axis_index("slab")}

    def bit_of(bit):
        return (me[bit[0]] // bit[1]) % 2

    def partner(bit):
        there = dict(me)
        there[bit[0]] = me[bit[0]] + bit[1] * (1 - 2 * bit_of(bit))
        return (there["dp"], there["slab"])

    barrier = pltpu.get_barrier_semaphore()
    for bit, _, _ in plan[0][2]:
        pl.semaphore_signal(barrier, inc=1, device_id=partner(bit), device_id_type=MESH)
    pl.semaphore_wait(barrier, stages)

    first = [[start] for start, _, _ in plan]

    def window(start, length):
        return pl.ds(pl.multiple_of(start, 8), length)

    def begin(n, s):
        bit, length, halves = plan[n][2][s]
        before = first[n][s]
        mine = before + bit_of(bit) * length if halves else before
        other = before + (1 - bit_of(bit)) * length if halves else before
        first[n].append(mine)
        source = value if s == 0 else work
        copy = pltpu.make_async_remote_copy(
            src_ref=source.at[window(other, length)],
            dst_ref=recv[n][s],
            send_sem=send_sem.at[0, n, s],
            recv_sem=recv_sem.at[0, n, s],
            device_id=partner(bit),
            device_id_type=MESH,
        )
        copy.start()
        return copy

    flying = [begin(n, 0) for n in range(len(plan))]
    for s in range(stages):
        for n in range(len(plan)):
            _, length, _ = plan[n][2][s]
            flying[n].wait()
            here = window(first[n][s + 1], length)
            source = value if s == 0 else work
            target = work if s + 1 < stages else out
            target[here, :] = source[here, :] + recv[n][s][...]
            if s + 1 < stages:
                flying[n] = begin(n, s + 1)

    def spread(n, s):
        bit, length, _ = plan[n][2][s]
        here = window(first[n][s + 1], length)
        copy = pltpu.make_async_remote_copy(
            src_ref=out.at[here],
            dst_ref=out.at[here],
            send_sem=send_sem.at[1, n, s],
            recv_sem=recv_sem.at[1, n, s],
            device_id=partner(bit),
            device_id_type=MESH,
        )
        copy.start()
        return copy

    back = [[s for s in range(stages - 1, -1, -1) if stage[2][s][2]] for stage in plan]
    flying = [spread(n, back[n][0]) for n in range(len(plan))]
    for step in range(max(len(b) for b in back)):
        for n in range(len(plan)):
            if step < len(back[n]):
                flying[n].wait()
                if step + 1 < len(back[n]):
                    flying[n] = spread(n, back[n][step + 1])


def sum_everywhere(value):
    rows, lanes = value.shape
    plan = portion_plan(rows, bit_orders(lax.axis_size("dp"), lax.axis_size("slab")))
    stages = len(plan[0][2])
    buffers = [
        pltpu.VMEM((length, lanes), value.dtype) for _, _, steps in plan for _, length, _ in steps
    ]
    return pl.pallas_call(
        functools.partial(sum_kernel, plan),
        out_shape=jax.ShapeDtypeStruct(value.shape, value.dtype),
        in_specs=[pl.BlockSpec(memory_space=pltpu.VMEM)],
        out_specs=pl.BlockSpec(memory_space=pltpu.VMEM),
        scratch_shapes=[pltpu.VMEM(value.shape, value.dtype)]
        + buffers
        + [pltpu.SemaphoreType.DMA((2, len(plan), stages))] * 2,
        compiler_params=pltpu.CompilerParams(
            collective_id=0, has_side_effects=True, vmem_limit_bytes=24 * 1024 * 1024
        ),
        name="sum_everywhere",
    )(value)


def halo_kernel(size, parts, own, swapped, relayed, send_sem, recv_sem):
    dp, me = lax.axis_index("dp"), lax.axis_index("slab")
    odd = me % 2
    mate = me + 1 - 2 * odd
    target = me + 2 - 4 * odd
    source = me - 2 + 4 * odd
    gives = (target >= 0) & (target < size)
    takes = (source >= 0) & (source < size)
    barrier = pltpu.get_barrier_semaphore()
    pl.semaphore_signal(barrier, inc=1, device_id=(dp, mate), device_id_type=MESH)

    @pl.when(gives)
    def _():
        pl.semaphore_signal(barrier, inc=1, device_id=(dp, target), device_id_type=MESH)

    @pl.when(takes)
    def _():
        pl.semaphore_signal(barrier, inc=1, device_id=(dp, source), device_id_type=MESH)

    pl.semaphore_wait(barrier, 1 + gives.astype(jnp.int32) + takes.astype(jnp.int32))
    step = own.shape[1] // parts

    def piece(kind, n):
        here = slice(n * step, (n + 1) * step)
        return pltpu.make_async_remote_copy(
            src_ref=(own if kind == 0 else swapped).at[:, here],
            dst_ref=(swapped if kind == 0 else relayed).at[:, here],
            send_sem=send_sem.at[kind, n],
            recv_sem=recv_sem.at[kind, n],
            device_id=(dp, mate if kind == 0 else target),
            device_id_type=MESH,
        )

    for n in range(parts):
        piece(0, n).start()

    @pl.when(jnp.logical_not(takes))
    def _():
        relayed[...] = jnp.zeros_like(relayed)

    for n in range(parts):
        piece(0, n).wait_recv()

        @pl.when(gives)
        def _():
            piece(1, n).start()

    for n in range(parts):
        piece(0, n).wait_send()

        @pl.when(gives)
        def _():
            piece(1, n).wait_send()

        @pl.when(takes)
        def _():
            piece(1, n).wait_recv()


def halo(plane):
    size, parts = lax.axis_size("slab"), 16
    swapped, relayed = pl.pallas_call(
        functools.partial(halo_kernel, size, parts),
        out_shape=[jax.ShapeDtypeStruct(plane.shape, plane.dtype)] * 2,
        in_specs=[pl.BlockSpec(memory_space=pltpu.VMEM)],
        out_specs=[pl.BlockSpec(memory_space=pltpu.VMEM)] * 2,
        scratch_shapes=[pltpu.SemaphoreType.DMA((2, parts))] * 2,
        compiler_params=pltpu.CompilerParams(
            collective_id=1, has_side_effects=True, vmem_limit_bytes=16 * 1024 * 1024
        ),
        name="halo",
    )(plane)
    return swapped, relayed


def shards(acts, grads, picks):
    volumes, channels, planes, height, width = acts.shape
    outputs = grads.shape[1]
    cells = height * width
    own = acts.reshape(channels, cells)
    rows = grads.reshape(outputs, cells)
    swapped, relayed = halo(own)
    samples = picks.shape[1]
    chunks = cells // CHUNK
    position = jnp.arange(samples, dtype=jnp.int32) * 32 + picks.reshape(samples)
    column = position % width
    targets = jnp.stack(
        [
            jnp.where((column + d >= 0) & (column + d < width), position + d, -1)
            for d in (-1, 0, 1)
        ]
    )
    targets = targets.reshape(3, chunks, samples // chunks).transpose(0, 2, 1)
    targets = targets.reshape(3 * (samples // chunks), chunks)
    size = 27 * channels + outputs
    count = size // BLOCK
    blocks = count * (count + 1) // 2
    partial = pl.pallas_call(
        functools.partial(local_kernel, width),
        out_shape=jax.ShapeDtypeStruct((blocks, BLOCK, BLOCK), jnp.float32),
        in_specs=[pl.BlockSpec(memory_space=pltpu.VMEM)] * 5,
        out_specs=pl.BlockSpec(memory_space=pltpu.VMEM),
        scratch_shapes=[
            pltpu.VMEM((3 * channels, cells + 2 * width), jnp.bfloat16),
            pltpu.VMEM((size, samples), jnp.float32),
            pltpu.VMEM((size, BLOCK), jnp.float32),
        ],
        compiler_params=pltpu.CompilerParams(vmem_limit_bytes=48 * 1024 * 1024),
        name="local_sums",
    )(own, swapped, relayed, rows, targets)
    total = sum_everywhere(partial.reshape(-1, BLOCK)).reshape(partial.shape)
    everyone = lax.axis_size("dp") * lax.axis_size("slab") * volumes
    return pl.pallas_call(
        functools.partial(
            solve_kernel, everyone * planes * cells, everyone * samples, channels, outputs
        ),
        out_shape=[jax.ShapeDtypeStruct((outputs, 27 * channels), jnp.float32)] * 2,
        in_specs=[pl.BlockSpec(memory_space=pltpu.VMEM)],
        out_specs=[pl.BlockSpec(memory_space=pltpu.VMEM)] * 2,
        scratch_shapes=[pltpu.VMEM((size, size), jnp.bfloat16)] * 3
        + [pltpu.VMEM((size, 3 * outputs), jnp.bfloat16)]
        + [pltpu.VMEM((size, outputs), jnp.float32)] * 4
        + [pltpu.VMEM((size, 1), jnp.float32)],
        compiler_params=pltpu.CompilerParams(vmem_limit_bytes=48 * 1024 * 1024),
        name="solve",
    )(total)


def solution(mesh):
    return jax.shard_map(
        shards,
        mesh=mesh,
        in_specs=(
            P("dp", None, "slab", None, None),
            P("dp", None, "slab", None, None),
            P("dp", "slab"),
        ),
        out_specs=(P(), P()),
        check_vma=False,
    )
```
